32 devices in a mesh: ent: 16 (over z, y, x), dim: 2 (over core).
Axes of the slice: x: 2, y: 2, z: 4, core: 2. Of those that a mesh axis runs over, the one named last changes fastest.
Arguments:
- entities: float32 [32768, 1024], P('ent', 'dim'), may hold values from -3 to 3
- ent_state: float32 [32768], P('ent'), may hold values from 0.01 to 0.1
- buckets: int32 [32768], P('ent'), may hold values from 0 to 7
- relations: float32 [4096, 1024], P(None, 'dim'), may hold values from -1.6 to 1.6
- rel_state: float32 [4096], replicated, may hold values from 0.05 to 0.5
- triples: int32 [3, 8192], P(None, 'ent'), may hold values from 0 to 32767, as said below
- negatives: int32 [32, 256], P('ent'), may hold values from 0 to 32767, as said below
Outputs:
- new_entities: float32 [32768, 1024], P('ent', 'dim')
- new_relations: float32 [4096, 1024], P(None, 'dim')
The draws below stay inside these ranges and needn't reach their ends.
Inputs may be any that keep to these rules, and one draw needn't show every extreme that they name: `triples`: rows 0 and 2 hold entity ids, row 1 relation ids below 4096. The block of an entity id is id // 2048. Among the 768 ids of one group (its heads, its tails and its negatives) at most 128 lie in one block, and in every draw, for each rank of a group among the 2 groups of an index of ent, some block holds exactly 128 ids of that group on every index of ent. `negatives`: entity ids; they count in the bound on the ids of a group stated for triples.
All inputs are finite; a program needn't handle non-finite values.
Results may differ from the reference program's by a relative error of at most 0.0017.
Values may be sent and summed in bfloat16 or wider, within the bound.
A program may use at most 128 MiB of HBM per device.

```python
import math
import jax
import jax.numpy as jnp
from jax import lax

RANK = 512
BLK = 64
NREL = 4096
NEG = 256
GROUP = 256
NBUCK = 8
GROUP_DEV = 2
ENT_DEV = 2048
NENT = 32768
GROUPS = 32
TRIPLES = 8192
REQC = 768
CAPC = 128


def group_entity_ids(key):
    owner_count = NENT // ENT_DEV
    labels = jnp.repeat(jnp.arange(owner_count, dtype=jnp.int32), CAPC)
    star_owner = jax.random.randint(jax.random.fold_in(key, 11), (GROUP_DEV,), 0, owner_count)

    def one_group(group_key, full_owner):
        first_key, second_key, third_key, fourth_key = jax.random.split(group_key, 4)
        scores = jax.random.permutation(first_key, owner_count * CAPC).astype(jnp.int32)
        scores = jnp.where(labels == full_owner, scores - owner_count * CAPC, scores)
        order = jnp.argsort(scores, stable=True)
        chosen = labels[order[:REQC]]
        chosen = chosen[jax.random.permutation(second_key, REQC)]
        upper = jax.random.randint(third_key, (REQC,), 1, ENT_DEV + 1)
        local_rows = jax.random.randint(fourth_key, (REQC,), 0, upper)
        return chosen * ENT_DEV + local_rows
    group_keys = jax.random.split(jax.random.fold_in(key, 7), GROUPS)
    full_owners = star_owner[jnp.arange(GROUPS) % GROUP_DEV]
    return jax.vmap(one_group)(group_keys, full_owners).astype(jnp.int32)


def draw_triples(key, part):
    entity_ids = group_entity_ids(key)
    head_ids = entity_ids[:, :GROUP].reshape(TRIPLES)
    tail_ids = entity_ids[:, GROUP:2 * GROUP].reshape(TRIPLES)
    upper = jax.random.randint(jax.random.fold_in(key, 13), (TRIPLES,), 1, NREL + 1)
    rel_ids = jax.random.randint(jax.random.fold_in(key, 17), (TRIPLES,), 0, upper)
    return jnp.stack([head_ids, rel_ids.astype(jnp.int32), tail_ids], axis=0)


def draw_negatives(key, part):
    entity_ids = group_entity_ids(key)
    return entity_ids[:, 2 * GROUP:]


def touch_ends(values, own_key, smallest, high):
    spot = [jax.random.randint(jax.random.fold_in(own_key, axis), (), 0, length) for axis, length in enumerate(values.shape)]
    main_axis = values.shape.index(max(values.shape))
    next_to = spot[:main_axis] + [(spot[main_axis] + 1) % values.shape[main_axis]] + spot[main_axis + 1:]
    return values.at[tuple(spot)].set(smallest).at[tuple(next_to)].set(high)


def shard_levels(stream_key, extent, pieces, smallest, high):
    def one(position, blocks):
        heights = jax.random.uniform(jax.random.fold_in(jax.random.fold_in(stream_key, 6), position), (blocks,), jnp.float32, smallest / len(pieces), high / len(pieces))
        return jnp.repeat(jnp.exp(heights), extent[position] // blocks).reshape((-1,) + (1,) * (len(extent) - position - 1))

    gain = one(*pieces[0])
    for cut in pieces[1:]:
        gain = gain * one(*cut)
    return gain


def noise(key, shape, scale, bound, pieces=(), kind=jnp.bfloat16):
    array = jax.random.normal(key, shape, jnp.float32) * scale
    if len(pieces) > 0:
        array = shard_levels(key, shape, pieces, -0.22, 0.18) * array
    return jnp.clip(array, min=-bound, max=bound).astype(kind)


def setup_inputs(seed: int = 0) -> dict:
    splits = jax.random.split(jax.random.key(seed), 8)
    entities = noise(splits[0], (NENT, 2 * RANK), 0.5, 3.0, ((0, 16), (1, 2)), jnp.float32)
    ent_state = jnp.clip(jnp.exp(math.log(0.1) - 2.3025851 * jax.random.uniform(splits[1], (NENT,), jnp.float32) ** shard_levels(splits[1], (NENT,), ((0, 16),), -0.2, 0.2)), 0.01, 0.1)
    buckets = touch_ends(jax.random.randint(splits[2], (NENT,), 0, NBUCK), jax.random.fold_in(splits[2], 1), 0, NBUCK - 1).astype(jnp.int32)
    relations = noise(splits[3], (NREL, 2 * RANK), 0.27, 1.6, ((1, 2),), jnp.float32)
    rel_state = jnp.clip(jnp.exp(jax.random.uniform(splits[4], (NREL,), jnp.float32, math.log(0.05), math.log(0.5))), 0.05, 0.5)
    triples = draw_triples(jax.random.fold_in(splits[7], 71), 0)
    negatives = draw_negatives(jax.random.fold_in(splits[7], 71), 0)
    return {"entities": entities, "ent_state": ent_state, "buckets": buckets, "relations": relations, "rel_state": rel_state, "triples": triples, "negatives": negatives}


LEARN_RATE = 0.1
REG_WEIGHT = 0.01

def halves(values):
    shaped = values.reshape(values.shape[:-1] + (values.shape[-1] // (2 * BLK), 2, BLK))
    return (shaped[..., 0, :], shaped[..., 1, :])

def joined(real_part, imag_part):
    stacked = jnp.stack([real_part, imag_part], axis=-2)
    return stacked.reshape(stacked.shape[:-3] + (stacked.shape[-3] * 2 * BLK,))

def complex_product(former, latter):
    former_re, former_im = halves(former)
    latter_re, latter_im = halves(latter)
    return joined(former_re * latter_re - former_im * latter_im, former_re * latter_im + former_im * latter_re)

def conjugate(values):
    real_part, imag_part = halves(values)
    return joined(real_part, -imag_part)

def rounded_back(values):
    return lax.optimization_barrier(values.astype(jnp.bfloat16)).astype(jnp.float32)

def adagrad(table, state, grad):
    new_state = state + lax.optimization_barrier(jnp.mean(grad * grad, axis=-1))
    return table - LEARN_RATE * grad / jnp.sqrt(new_state)[:, None]

def reference(entities, ent_state, buckets, relations, rel_state, triples, negatives):
    ent_low = lax.optimization_barrier(entities.astype(jnp.bfloat16))
    rel_low = lax.optimization_barrier(relations.astype(jnp.bfloat16))
    head_ids = triples[0]
    rel_ids = triples[1]
    tail_ids = triples[2]
    head_rows = ent_low[head_ids].astype(jnp.float32)
    tail_rows = ent_low[tail_ids].astype(jnp.float32)
    rel_rows = rel_low[rel_ids].astype(jnp.float32)
    noise_rows = ent_low[negatives].astype(jnp.float32)
    query = rounded_back(complex_product(head_rows, rel_rows))
    probe = rounded_back(complex_product(conjugate(rel_rows), tail_rows))
    pos_score = lax.optimization_barrier(jnp.sum(query * tail_rows, axis=-1))
    query_groups = query.reshape(GROUPS, GROUP, 2 * RANK)
    probe_groups = probe.reshape(GROUPS, GROUP, 2 * RANK)
    tail_score = jnp.einsum('cid,cnd->cin', query_groups, noise_rows)
    head_score = jnp.einsum('cid,cnd->cin', probe_groups, noise_rows)
    pos_coef = rounded_back(-jax.nn.sigmoid(-pos_score))
    tail_coef = rounded_back(jax.nn.sigmoid(tail_score) / NEG)
    head_coef = rounded_back(jax.nn.sigmoid(head_score) / NEG)
    tail_pull = pos_coef[:, None] * tail_rows + jnp.einsum('cin,cnd->cid', tail_coef, noise_rows).reshape(TRIPLES, 2 * RANK)
    head_pull = jnp.einsum('cin,cnd->cid', head_coef, noise_rows).reshape(TRIPLES, 2 * RANK)
    head_side = pos_coef[:, None] * head_rows + head_pull
    head_grad = complex_product(conjugate(rel_rows), tail_pull).astype(jnp.bfloat16)
    tail_grad = complex_product(rel_rows, head_side).astype(jnp.bfloat16)
    noise_grad = (jnp.einsum('cin,cid->cnd', tail_coef, query_groups) + jnp.einsum('cin,cid->cnd', head_coef, probe_groups)).astype(jnp.bfloat16)
    rel_grad_rows = complex_product(conjugate(head_rows), tail_pull) + complex_product(tail_rows, conjugate(head_pull))
    all_ids = jnp.concatenate([head_ids, tail_ids, negatives.reshape(-1)]).astype(jnp.int32)
    all_grads = jnp.concatenate([head_grad, tail_grad, noise_grad.reshape(GROUPS * NEG, 2 * RANK)], axis=0).astype(jnp.float32)
    ent_grad = jnp.zeros((NENT, 2 * RANK), jnp.float32).at[all_ids].add(all_grads)
    counts = jnp.zeros((NENT,), jnp.float32).at[all_ids].add(jnp.ones(all_ids.shape, jnp.float32))
    weight = REG_WEIGHT * (buckets.astype(jnp.float32) + 1.0) * counts
    ent_grad = ent_grad + weight[:, None] * 3.0 * entities * jnp.abs(entities)
    rel_grad = jnp.zeros((NREL, 2 * RANK), jnp.float32).at[rel_ids].add(rel_grad_rows)
    return (adagrad(entities, ent_state, ent_grad), adagrad(relations, rel_state, rel_grad))
```

```python
import functools

import jax
import jax.numpy as jnp
from jax import lax
from jax.experimental import pallas as pl
from jax.experimental.pallas import tpu as pltpu
from jax.sharding import PartitionSpec as P

RANK = 512
BLK = 64


LEARN_RATE = 0.1
REG_WEIGHT = 0.01
MESH = pl.DeviceIdType.MESH


def halves(values):
    shaped = values.reshape(values.shape[:-1] + (values.shape[-1] // (2 * BLK), 2, BLK))
    return (shaped[..., 0, :], shaped[..., 1, :])


def joined(real_part, imag_part):
    stacked = jnp.stack([real_part, imag_part], axis=-2)
    return stacked.reshape(stacked.shape[:-3] + (stacked.shape[-3] * 2 * BLK,))


def complex_product(former, latter):
    former_re, former_im = halves(former)
    latter_re, latter_im = halves(latter)
    return joined(
        former_re * latter_re - former_im * latter_im, former_re * latter_im + former_im * latter_re
    )


def conjugate(values):
    real_part, imag_part = halves(values)
    return joined(real_part, -imag_part)


def rounded(values):
    return lax.optimization_barrier(values.astype(jnp.bfloat16))


def contract_first(former, latter):
    return lax.dot_general(
        former, latter, (((0,), (0,)), ((), ())), preferred_element_type=jnp.float32
    )


def contract_last(former, latter):
    return lax.dot_general(
        former, latter, (((1,), (1,)), ((), ())), preferred_element_type=jnp.float32
    )


def position(near_size):
    me = lax.axis_index("ent")
    return lax.div(me, near_size), lax.rem(me, near_size)


def greet(near_size, far_size):
    far, near = position(near_size)
    barrier = pltpu.get_barrier_semaphore()
    for step in range(1, near_size):
        peer = far * near_size + lax.rem(near + step, near_size)
        pl.semaphore_signal(barrier, inc=1, device_id={"ent": peer}, device_id_type=MESH)
    for step in range(1, far_size):
        peer = lax.rem(far + step, far_size) * near_size + near
        pl.semaphore_signal(barrier, inc=1, device_id={"ent": peer}, device_id_type=MESH)
    pl.semaphore_wait(barrier, near_size + far_size - 2)


def send(source, target, send_sem, recv_sem, peer):
    return pltpu.make_async_remote_copy(
        src_ref=source,
        dst_ref=target,
        send_sem=send_sem,
        recv_sem=recv_sem,
        device_id={"ent": peer},
        device_id_type=MESH,
    )


def line_step(index, far_size):
    return jnp.where(
        index == far_size - 1, 0, 1 + lax.rem(far_size // 2 - 1 + index, far_size - 1)
    )


def fetch_kernel(
    sizes, table, ids, maps, arrived, own_ids, line_maps,
    line_ids, near_out, near_in, far_out,
    ids_ss, ids_rs, maps_ss, maps_rs, fwd_ss, fwd_rs, near_ss, near_rs, far_ss, far_rs,
):
    near_size, far_size, groups, slots, merged = sizes
    far, near = position(near_size)
    rows_here = table.shape[0]
    greet(near_size, far_size)

    def line_peer(step):
        there = lax.rem(far + step, far_size)
        return there, there * near_size + near

    def ids_copy(step):
        there, peer = line_peer(step)
        return send(ids.at[there], line_ids.at[far], ids_ss.at[step], ids_rs.at[step], peer)

    def maps_copy(step):
        there, peer = line_peer(step)
        return send(maps.at[there], line_maps.at[far], maps_ss.at[step], maps_rs.at[step], peer)

    def near_peer(step):
        there = lax.rem(near + step, near_size)
        return there, far * near_size + there

    def fwd_copy(step):
        there, peer = near_peer(step)
        return send(
            line_ids.at[:, there], own_ids.at[near], fwd_ss.at[step], fwd_rs.at[step], peer
        )

    for step in range(1, far_size):
        ids_copy(step).start()
    for step in range(1, far_size):
        maps_copy(step).start()
    line_ids[far] = ids[far]
    line_maps[far] = maps[far]
    for step in range(1, far_size):
        ids_copy(step).wait()
    for step in range(1, near_size):
        fwd_copy(step).start()
    own_ids[near] = line_ids[:, near]
    for step in range(1, near_size):
        fwd_copy(step).wait()
    for step in range(1, far_size):
        maps_copy(step).wait()

    def near_copy(group, step, there):
        beside, peer = near_peer(step)
        return send(
            near_out.at[group, step, there],
            near_in.at[group, there, near],
            near_ss.at[group, step, there],
            near_rs.at[group, step, there],
            peer,
        )

    def look_up(group, index):
        step = lax.rem(index + 1, near_size)
        there = lax.rem(far + line_step(lax.div(index, near_size), far_size), far_size)
        beside = lax.rem(near + step, near_size)
        wanted = jnp.transpose(own_ids[beside, there])[:slots, group : group + 1]
        hits = (wanted == lax.broadcasted_iota(jnp.int32, (slots, rows_here), 1))
        found = jnp.dot(
            hits.astype(jnp.float32).astype(jnp.bfloat16), table[...], preferred_element_type=jnp.float32
        ).astype(jnp.bfloat16)

        @pl.when(step == 0)
        def _():
            near_in[group, there, near] = found

        @pl.when(step != 0)
        def _():
            near_out[group, step, there] = found
            near_copy(group, step, there).start()

    def far_copy(group, there):
        peer = there * near_size + near
        return send(
            far_out.at[group, there],
            arrived.at[group, far],
            far_ss.at[group, there],
            far_rs.at[group, far],
            peer,
        )

    def far_arrival(group, there):
        peer = there * near_size + near
        return send(
            far_out.at[group, there],
            arrived.at[group, there],
            far_ss.at[group, there],
            far_rs.at[group, there],
            peer,
        )

    def merge(group, index):
        there = lax.rem(far + line_step(index, far_size), far_size)
        for step in range(1, near_size):
            near_copy(group, step, there).wait_recv()
        targets = line_maps[there][group : group + 1]
        picks = (
            lax.broadcasted_iota(jnp.int32, (merged, near_size * slots), 0) == targets
        )
        rows = near_in[group, there].reshape(near_size * slots, table.shape[1])
        block = jnp.dot(
            picks.astype(jnp.float32).astype(jnp.bfloat16), rows, preferred_element_type=jnp.float32
        ).astype(jnp.bfloat16)

        @pl.when(there == far)
        def _():
            arrived[group, far] = block

        @pl.when(there != far)
        def _():
            far_out[group, there] = block
            far_copy(group, there).start()

    @pl.loop(0, far_size * near_size)
    def _(index):
        look_up(0, index)

    for group in range(1, groups):

        @pl.loop(0, far_size)
        def _(index):
            @pl.loop(0, near_size)
            def _(part):
                look_up(group, index * near_size + part)

            merge(group - 1, index)

    @pl.loop(0, far_size)
    def _(index):
        merge(groups - 1, index)

    for group in range(groups):
        for step in range(1, far_size):
            there = lax.rem(far + step, far_size)
            far_arrival(group, there).wait()
        for step in range(1, near_size):

            @pl.loop(0, far_size)
            def _(there):
                near_copy(group, step, there).wait_send()


def fetch(table, ids, maps, sizes):
    near_size, far_size, groups, slots, merged = sizes
    columns = table.shape[1]
    dma = pltpu.SemaphoreType.DMA
    vmem = pl.BlockSpec(memory_space=pltpu.VMEM)
    return pl.pallas_call(
        functools.partial(fetch_kernel, sizes),
        name="fetch_rows",
        out_shape=(
            jax.ShapeDtypeStruct((groups, far_size, merged, columns), jnp.bfloat16),
            jax.ShapeDtypeStruct((near_size,) + ids.shape[:1] + ids.shape[2:], jnp.int32),
            jax.ShapeDtypeStruct(maps.shape, jnp.int32),
        ),
        in_specs=[vmem] * 3,
        out_specs=(vmem,) * 3,
        scratch_shapes=[
            pltpu.VMEM(ids.shape, jnp.int32),
            pltpu.VMEM((groups, near_size, far_size, slots, columns), jnp.bfloat16),
            pltpu.VMEM((groups, far_size, near_size, slots, columns), jnp.bfloat16),
            pltpu.VMEM((groups, far_size, merged, columns), jnp.bfloat16),
            dma((far_size,)), dma((far_size,)), dma((far_size,)), dma((far_size,)),
            dma((near_size,)), dma((near_size,)),
            dma((groups, near_size, far_size)), dma((groups, near_size, far_size)),
            dma((groups, far_size)), dma((groups, far_size)),
        ],
        compiler_params=pltpu.CompilerParams(
            collective_id=0, has_side_effects=True, vmem_limit_bytes=48 * 1024 * 1024
        ),
    )(table, ids, maps)


def give_back_kernel(
    sizes, blocks, own_ids, maps_down, totals,
    far_in, near_out, near_in, far_ss, far_rs, near_ss, near_rs,
):
    near_size, far_size, groups, slots, merged = sizes
    far, near = position(near_size)
    rows_here, columns = totals.shape
    greet(near_size, far_size)

    def far_copy(group, step):
        there = lax.rem(far + step, far_size)
        return send(
            blocks.at[group, there],
            far_in.at[group, far],
            far_ss.at[group, step],
            far_rs.at[group, far],
            there * near_size + near,
        )

    def far_arrival(group, there):
        return send(
            blocks.at[group, there],
            far_in.at[group, there],
            far_ss.at[group, 0],
            far_rs.at[group, there],
            there * near_size + near,
        )

    def near_copy(group, step, there):
        beside = lax.rem(near + step, near_size)
        return send(
            near_out.at[group, there, beside],
            near_in.at[group, near, there],
            near_ss.at[group, step, there],
            near_rs.at[group, step, there],
            far * near_size + beside,
        )

    for group in range(groups):

        @pl.loop(0, far_size - 1)
        def _(index):
            far_copy(group, line_step(index, far_size)).start()

    totals[...] = jnp.zeros_like(totals)

    def spread(group, index):
        step = lax.rem(index, far_size)
        there = lax.rem(far + step, far_size)

        @pl.when(step == 0)
        def _():
            far_in[group, far] = blocks[group, far]

        @pl.when(step != 0)
        def _():
            far_arrival(group, there).wait_recv()

        targets = maps_down[there][:, group : group + 1]
        picks = lax.broadcasted_iota(jnp.int32, (near_size * slots, merged), 1) == targets
        rows = jnp.dot(
            picks.astype(jnp.float32).astype(jnp.bfloat16), far_in[group, there],
            preferred_element_type=jnp.float32,
        ).astype(jnp.bfloat16)
        near_out[group, there] = rows.reshape(near_size, slots, columns)
        for step in range(1, near_size):
            near_copy(group, step, there).start()
        near_in[group, near, there] = near_out[group, there, near]

    def add_up(group, step):
        beside = lax.rem(near + near_size - step, near_size)

        @pl.when(step != 0)
        def _():
            @pl.loop(0, far_size)
            def _(there):
                near_copy(group, step, there).wait_recv()

        targets = own_ids[beside][group : group + 1]
        hits = lax.broadcasted_iota(jnp.int32, (rows_here, far_size * slots), 0) == targets
        rows = near_in[group, beside].reshape(far_size * slots, columns)
        totals[...] += jnp.dot(
            hits.astype(jnp.float32).astype(jnp.bfloat16), rows, preferred_element_type=jnp.float32
        )

    for group in range(groups):

        @pl.loop(0, far_size)
        def _(index):
            spread(group, index)

    for group in range(groups):

        @pl.loop(0, near_size)
        def _(step):
            add_up(group, step)

    for group in range(groups):
        for step in range(1, far_size):
            far_copy(group, step).wait_send()
        for step in range(1, near_size):

            @pl.loop(0, far_size)
            def _(there):
                near_copy(group, step, there).wait_send()


def give_back(blocks, own_ids, maps_down, rows_here, sizes):
    near_size, far_size, groups, slots, merged = sizes
    columns = blocks.shape[-1]
    dma = pltpu.SemaphoreType.DMA
    vmem = pl.BlockSpec(memory_space=pltpu.VMEM)
    return pl.pallas_call(
        functools.partial(give_back_kernel, sizes),
        name="give_back_rows",
        out_shape=jax.ShapeDtypeStruct((rows_here, columns), jnp.float32),
        in_specs=[vmem] * 3,
        out_specs=vmem,
        scratch_shapes=[
            pltpu.VMEM((groups, far_size, merged, columns), jnp.bfloat16),
            pltpu.VMEM((groups, far_size, near_size, slots, columns), jnp.bfloat16),
            pltpu.VMEM((groups, near_size, far_size, slots, columns), jnp.bfloat16),
            dma((groups, far_size)), dma((groups, far_size)),
            dma((groups, near_size, far_size)), dma((groups, near_size, far_size)),
        ],
        compiler_params=pltpu.CompilerParams(
            collective_id=1, has_side_effects=True, vmem_limit_bytes=48 * 1024 * 1024
        ),
    )(blocks, own_ids, maps_down)


def group_step(rows_group, rel_float, group_len):
    head_float = rows_group[:group_len].astype(jnp.float32)
    tail_float = rows_group[group_len : 2 * group_len].astype(jnp.float32)
    noise_rows = rows_group[2 * group_len :]
    width_neg = noise_rows.shape[0]
    query = rounded(complex_product(head_float, rel_float))
    probe = rounded(complex_product(conjugate(rel_float), tail_float))
    part_pos = jnp.sum(query.astype(jnp.float32) * tail_float, axis=-1, keepdims=True)
    part = jnp.concatenate(
        [
            contract_last(query, noise_rows),
            contract_last(probe, noise_rows),
            jnp.broadcast_to(part_pos, (group_len, 128)),
        ],
        axis=1,
    ).astype(jnp.bfloat16)
    scores = jnp.sum(lax.all_gather(part, "dim").astype(jnp.float32), axis=0)
    both_coef = rounded(jax.nn.sigmoid(scores[:, : 2 * width_neg]) / width_neg)
    pos_float = -jax.nn.sigmoid(-scores[:, 2 * width_neg : 2 * width_neg + 1])
    pos_float = rounded(pos_float).astype(jnp.float32)
    tail_coef = both_coef[:, :width_neg]
    head_coef = both_coef[:, width_neg:]
    tail_pull = pos_float * tail_float + jnp.dot(
        tail_coef, noise_rows, preferred_element_type=jnp.float32
    )
    head_pull = jnp.dot(head_coef, noise_rows, preferred_element_type=jnp.float32)
    head_side = pos_float * head_float + head_pull
    head_grad = complex_product(conjugate(rel_float), tail_pull).astype(jnp.bfloat16)
    tail_grad = complex_product(rel_float, head_side).astype(jnp.bfloat16)
    noise_grad = (contract_first(tail_coef, query) + contract_first(head_coef, probe)).astype(
        jnp.bfloat16
    )
    rel_grad = complex_product(conjugate(head_float), tail_pull) + complex_product(
        tail_float, conjugate(head_pull)
    )
    return (
        jnp.concatenate([head_grad, tail_grad, noise_grad], axis=0),
        rel_grad.astype(jnp.bfloat16),
    )


def placement_of(wanted_row, rows_here, sizes):
    near_size, far_size, _, slots, merged = sizes
    owners = near_size * far_size
    request_count = wanted_row.shape[0]
    owner_of = wanted_row // rows_here
    owner_hits = (owner_of[:, None] == jnp.arange(owners, dtype=jnp.int32)[None, :]).astype(
        jnp.bfloat16
    )
    order = jnp.arange(request_count, dtype=jnp.int32)
    earlier = (order[:, None] > order[None, :]).astype(jnp.bfloat16)
    before = jnp.dot(earlier, owner_hits, preferred_element_type=jnp.float32)
    slot_rank = jnp.sum(before * owner_hits.astype(jnp.float32), axis=-1).astype(jnp.int32)
    plane_of = owner_of // near_size
    same_plane = (
        plane_of[:, None] == (jnp.arange(owners, dtype=jnp.int32) // near_size)[None, :]
    ).astype(jnp.float32)
    plane_rank = jnp.sum(before * same_plane, axis=-1).astype(jnp.int32)
    slot_flat = owner_of * slots + slot_rank
    at_slot = slot_flat[:, None] == jnp.arange(owners * slots, dtype=jnp.int32)[None, :]
    local_row = wanted_row - owner_of * rows_here
    slot_ids = jnp.sum(jnp.where(at_slot, local_row[:, None] + 1, 0), axis=0) - 1
    slot_map = jnp.sum(jnp.where(at_slot, plane_rank[:, None] + 1, 0), axis=0) - 1
    merged_flat = plane_of * merged + plane_rank
    matches = merged_flat[:, None] == jnp.arange(far_size * merged, dtype=jnp.int32)[None, :]
    return (matches.astype(jnp.bfloat16), slot_ids, slot_map)


def teams(near_size, far_size):
    near = [[row * near_size + place for place in range(near_size)] for row in range(far_size)]
    far = [[row * near_size + place for row in range(far_size)] for place in range(near_size)]
    return (near, far)


def sum_relations(rel_rows, near_ids, rel_count, near, far):
    near_size, far_size = len(far), len(near)
    row_count, columns = rel_rows.shape
    tiles = rel_rows.reshape(row_count, near_size, columns // near_size).transpose(1, 0, 2)
    tiles = lax.all_to_all(
        tiles, "ent", split_axis=0, concat_axis=0, axis_index_groups=near, tiled=True
    )
    hits = (near_ids[:, None] == jnp.arange(rel_count, dtype=jnp.int32)[None, :]).astype(
        jnp.bfloat16
    )
    part = contract_first(hits, tiles.reshape(near_size * row_count, columns // near_size)).astype(
        jnp.bfloat16
    )
    share = lax.psum_scatter(
        part, "ent", scatter_dimension=0, axis_index_groups=far, tiled=True
    )
    whole = lax.all_gather(share, "ent", axis=0)
    whole = whole.reshape(far_size, near_size, rel_count // far_size, columns // near_size)
    return whole.transpose(0, 2, 1, 3).reshape(rel_count, columns).astype(jnp.float32)


def adagrad(table, state, grad, squares):
    new_state = state + squares / (2 * RANK)
    scale = LEARN_RATE / jnp.sqrt(new_state)
    return table - grad * scale[:, None]


def per_device(entities, ent_state, buckets, relations, rel_state, triples, negatives):
    owners = lax.axis_size("ent")
    rows_here, columns_here = entities.shape
    rel_count = relations.shape[0]
    groups_here = negatives.shape[0]
    group_len = triples.shape[1] // groups_here
    request_count = 2 * group_len + negatives.shape[1]
    slots = 8 * ((request_count + 3 * owners - 1) // (3 * owners))
    near_size = 4 if owners % 4 == 0 else 1
    far_size = owners // near_size
    merged = near_size * slots
    sizes = (near_size, far_size, groups_here, slots, merged)
    ent_low = entities.astype(jnp.bfloat16)
    head_ids = triples[0].reshape(groups_here, group_len)
    tail_ids = triples[2].reshape(groups_here, group_len)
    wanted = jnp.concatenate([head_ids, tail_ids, negatives], axis=1)
    placed = [
        placement_of(wanted[index], rows_here, sizes) for index in range(groups_here)
    ]
    near, far = teams(near_size, far_size)
    near_ids = lax.all_gather(triples[1], "ent", axis_index_groups=near, tiled=True)
    slot_ids = jnp.stack([ids for _, ids, _ in placed])
    slot_ids = slot_ids.reshape(groups_here, far_size, near_size, slots).transpose(1, 2, 0, 3)
    slot_ids = jnp.pad(
        slot_ids, ((0, 0), (0, 0), (0, 8 - groups_here), (0, 128 - slots)), constant_values=-1
    )
    slot_maps = jnp.stack([maps for _, _, maps in placed])
    slot_maps = slot_maps.reshape(groups_here, far_size, near_size * slots).transpose(1, 0, 2)
    slot_maps = jnp.pad(
        slot_maps, ((0, 0), (0, 8 - groups_here), (0, 0)), constant_values=-1
    )
    arrived, own_ids, line_maps = fetch(ent_low, slot_ids, slot_maps, sizes)
    own_ids = own_ids[..., :slots].transpose(0, 2, 1, 3).reshape(
        near_size, 8, far_size * slots
    )
    maps_down = line_maps.transpose(0, 2, 1)
    rel_float = rounded(jnp.take(relations, triples[1], axis=0, mode="clip")).astype(jnp.float32)
    outgoing, rel_rows = [], []
    for index in range(groups_here):
        matches = placed[index][0]
        rows_group = jnp.dot(
            matches,
            arrived[index].reshape(far_size * merged, columns_here),
            preferred_element_type=jnp.float32,
        ).astype(jnp.bfloat16)
        grads, rel_row = group_step(
            rows_group, rel_float[index * group_len : (index + 1) * group_len], group_len
        )
        outgoing.append(
            contract_first(matches, grads)
            .astype(jnp.bfloat16)
            .reshape(far_size, merged, columns_here)
        )
        rel_rows.append(rel_row)
    totals = give_back(jnp.stack(outgoing), own_ids, maps_down, rows_here, sizes)
    rel_grad = sum_relations(jnp.concatenate(rel_rows, axis=0), near_ids, rel_count, near, far)
    positions = jnp.arange(rows_here, dtype=jnp.int32)
    flat_ids = own_ids[:, :groups_here].reshape(-1)
    counts = jnp.sum(
        (flat_ids[:, None] == positions[None, :]).astype(jnp.bfloat16), axis=0, dtype=jnp.float32
    )
    weight = REG_WEIGHT * (buckets.astype(jnp.float32) + 1.0) * counts
    totals = totals + weight[:, None] * 3.0 * entities * jnp.abs(entities)
    ent_squares = jnp.sum(totals * totals, axis=-1)
    ent_all, rel_all = lax.psum((ent_squares, jnp.sum(rel_grad * rel_grad, axis=-1)), "dim")
    new_relations = adagrad(relations, rel_state, rel_grad, rel_all)
    new_entities = adagrad(entities, ent_state, totals, ent_all)
    return (new_entities, new_relations)


def solution(mesh):
    placed = (
        P("ent", "dim"),
        P("ent"),
        P("ent"),
        P(None, "dim"),
        P(),
        P(None, "ent"),
        P("ent", None),
    )
    return jax.shard_map(
        per_device,
        mesh=mesh,
        in_specs=placed,
        out_specs=(P("ent", "dim"), P(None, "dim")),
        check_vma=False,
    )
```

```python
import functools

import jax
import jax.numpy as jnp
from jax import lax
from jax.experimental import pallas as pl
from jax.experimental.pallas import tpu as pltpu
from jax.sharding import PartitionSpec as P

RANK = 512
BLK = 64


LEARN_RATE = 0.1
REG_WEIGHT = 0.01
MESH = pl.DeviceIdType.MESH
VMEM_LIMIT = 60 * 1024 * 1024


def contract_first(former, latter):
    return lax.dot_general(
        former, latter, (((0,), (0,)), ((), ())), preferred_element_type=jnp.float32
    )


def contract_last(former, latter):
    return lax.dot_general(
        former, latter, (((1,), (1,)), ((), ())), preferred_element_type=jnp.float32
    )


def position(near_size):
    me = lax.axis_index("ent")
    return lax.div(me, near_size), lax.rem(me, near_size)


def greet(near_size, far_size):
    far, near = position(near_size)
    parts = lax.axis_size("dim")
    barrier = pltpu.get_barrier_semaphore()
    for step in range(1, parts):
        peer = lax.rem(lax.axis_index("dim") + step, parts)
        pl.semaphore_signal(barrier, inc=1, device_id={"dim": peer}, device_id_type=MESH)
    for step in range(1, near_size):
        peer = far * near_size + lax.rem(near + step, near_size)
        pl.semaphore_signal(barrier, inc=1, device_id={"ent": peer}, device_id_type=MESH)
    for step in range(1, far_size):
        peer = lax.rem(far + step, far_size) * near_size + near
        pl.semaphore_signal(barrier, inc=1, device_id={"ent": peer}, device_id_type=MESH)
    pl.semaphore_wait(barrier, near_size + far_size + parts - 3)


def send(source, target, send_sem, recv_sem, peer, axis="ent"):
    return pltpu.make_async_remote_copy(
        src_ref=source,
        dst_ref=target,
        send_sem=send_sem,
        recv_sem=recv_sem,
        device_id={axis: peer},
        device_id_type=MESH,
    )


def line_step(index, far_size):
    return jnp.where(
        index == far_size - 1, 0, 1 + lax.rem(far_size // 2 - 1 + index, far_size - 1)
    )


def one_hot(condition):
    return condition.astype(jnp.float32).astype(jnp.bfloat16)


def dot(former, latter):
    return jnp.dot(former, latter, preferred_element_type=jnp.float32)


def swapped(values):
    return pltpu.roll(values, BLK, 1)


def spread_parts(values):
    other = swapped(values)
    first = lax.broadcasted_iota(jnp.int32, values.shape, 1) < BLK
    return jnp.where(first, values, other), jnp.where(first, -other, values)


def times(former, parts):
    return former * parts[0] + swapped(former) * parts[1]


def times_conj(former, parts):
    return former * parts[0] - swapped(former) * parts[1]


def step_kernel(sizes, refs_in, refs_out, scratch):
    near_size, far_size, groups, slots, merged, group_len, width_neg, rel_count = sizes
    table, ids, maps, place_col, place_row, rel_rows, rel_ids = refs_in
    totals, counts, rel_out = refs_out
    s = scratch
    rows_here, columns = table.shape
    in_kernel_sum = "tiles_in" in s
    far, near = position(near_size)
    parts = lax.axis_size("dim")
    part_here = lax.axis_index("dim")
    greet(near_size, far_size)

    def line_peer(step):
        there = lax.rem(far + step, far_size)
        return there, there * near_size + near

    def near_peer(step):
        there = lax.rem(near + step, near_size)
        return there, far * near_size + there

    def ids_copy(step):
        there, peer = line_peer(step)
        return send(ids.at[there], s["line_ids"].at[far], s["ids_ss"].at[step], s["ids_rs"].at[step], peer)

    def maps_copy(step):
        there, peer = line_peer(step)
        return send(maps.at[there], s["line_maps"].at[far], s["maps_ss"].at[step], s["maps_rs"].at[step], peer)

    def fwd_copy(step):
        there, peer = near_peer(step)
        return send(
            s["line_ids"].at[:, there], s["own_ids"].at[near], s["fwd_ss"].at[step], s["fwd_rs"].at[step], peer
        )

    def rel_ids_copy(step):
        there, peer = near_peer(step)
        return send(rel_ids, s["plane_rel"].at[near], s["rid_ss"].at[step], s["rid_rs"].at[step], peer)

    for step in range(1, far_size):
        ids_copy(step).start()
    for step in range(1, far_size):
        maps_copy(step).start()
    if in_kernel_sum:
        for step in range(1, near_size):
            rel_ids_copy(step).start()
        s["plane_rel"][near] = rel_ids[...]
    s["line_ids"][far] = ids[far]
    s["line_maps"][far] = maps[far]
    for step in range(1, far_size):
        ids_copy(step).wait()
    for step in range(1, near_size):
        fwd_copy(step).start()
    s["own_ids"][near] = s["line_ids"][:, near]
    for step in range(1, near_size):
        fwd_copy(step).wait()
    for step in range(1, far_size):
        maps_copy(step).wait()

    def near_copy(group, step, there):
        beside, peer = near_peer(step)
        return send(
            s["near_out"].at[group, step, there], s["near_in"].at[group, there, near],
            s["near_ss"].at[group, step, there], s["near_rs"].at[group, step, there], peer,
        )

    def look_up(group, index):
        step = lax.rem(index + 1, near_size)
        there = lax.rem(far + line_step(lax.div(index, near_size), far_size), far_size)
        beside = lax.rem(near + step, near_size)
        wanted = jnp.transpose(s["own_ids"][beside, there])[:slots, group : group + 1]
        hits = wanted == lax.broadcasted_iota(jnp.int32, (slots, rows_here), 1)
        found = dot(one_hot(hits), table[...]).astype(jnp.bfloat16)

        @pl.when(step == 0)
        def _():
            s["near_in"][group, there, near] = found

        @pl.when(step != 0)
        def _():
            s["near_out"][group, step, there] = found
            near_copy(group, step, there).start()

    def far_copy(group, there, source):
        return send(
            s["far_out"].at[group, there], s["arrived"].at[group, source],
            s["far_ss"].at[group, there], s["far_rs"].at[group, source], there * near_size + near,
        )

    def merge(group, index):
        there = lax.rem(far + line_step(index, far_size), far_size)
        for step in range(1, near_size):
            near_copy(group, step, there).wait_recv()
        targets = s["line_maps"][there][group : group + 1]
        picks = lax.broadcasted_iota(jnp.int32, (merged, near_size * slots), 0) == targets
        rows = s["near_in"][group, there].reshape(near_size * slots, columns)
        block = dot(one_hot(picks), rows).astype(jnp.bfloat16)

        @pl.when(there == far)
        def _():
            s["arrived"][group, far] = block

        @pl.when(there != far)
        def _():
            s["far_out"][group, there] = block
            far_copy(group, there, far).start()

    def part_copy(group, step):
        peer = lax.rem(part_here + step, parts)
        return send(
            s["part_all"].at[group, part_here], s["part_all"].at[group, part_here],
            s["part_ss"].at[group, step], s["part_rs"].at[group, step], peer, axis="dim",
        )

    def tiles_copy(group, step):
        there, peer = near_peer(step)
        span = pl.ds(group * group_len, group_len)
        return send(
            s["tiles_out"].at[there, span], s["tiles_in"].at[near, span],
            s["tiles_ss"].at[group, step], s["tiles_rs"].at[group, step], peer,
        )

    def give_copy(group, there, source):
        return send(
            s["give_out"].at[group, there], s["give_in"].at[group, source],
            s["give_ss"].at[group, there], s["give_rs"].at[group, source], there * near_size + near,
        )

    lanes = 2 * BLK
    blocks = columns // lanes

    def compute(group):
        for step in range(1, far_size):
            far_copy(group, 0, lax.rem(far + step, far_size)).wait_recv()
        incoming = s["arrived"][group].reshape(far_size * merged, columns)
        request_count = 2 * group_len + width_neg
        rows = s["rows"]
        third = 256 if request_count % 256 == 0 else request_count
        for start in range(0, request_count, third):
            at = place_col[start : start + third, group : group + 1]
            picks = lax.broadcasted_iota(jnp.int32, (third, far_size * merged), 1) == at
            rows[start : start + third] = dot(one_hot(picks), incoming).astype(jnp.bfloat16)
        pos = jnp.zeros((group_len, 1), jnp.float32)
        for block in range(blocks):
            cut = slice(block * lanes, (block + 1) * lanes)
            head = rows[:group_len, cut].astype(jnp.float32)
            tail = rows[group_len : 2 * group_len, cut].astype(jnp.float32)
            rel = spread_parts(rel_rows[group * group_len : (group + 1) * group_len, cut].astype(jnp.float32))
            query = times(head, rel).astype(jnp.bfloat16)
            s["query"][:, cut] = query
            s["probe"][:, cut] = times_conj(tail, rel).astype(jnp.bfloat16)
            pos += jnp.sum(query.astype(jnp.float32) * tail, axis=1, keepdims=True)
        noise = rows[2 * group_len :]
        part = s["part_all"]
        part[group, part_here, :, :width_neg] = contract_last(s["query"][...], noise).astype(jnp.bfloat16)
        part[group, part_here, :, width_neg : 2 * width_neg] = contract_last(
            s["probe"][...], noise
        ).astype(jnp.bfloat16)
        part[group, part_here, :, 2 * width_neg :] = jnp.broadcast_to(pos, (group_len, 128)).astype(
            jnp.bfloat16
        )
        for step in range(1, parts):
            part_copy(group, step).start()
        for step in range(1, parts):
            part_copy(group, step).wait_recv()
        scores = part[group, 0].astype(jnp.float32)
        for other in range(1, parts):
            scores += part[group, other].astype(jnp.float32)
        tail_coef = jax.nn.sigmoid(scores[:, :width_neg]) * (1.0 / width_neg)
        head_coef = jax.nn.sigmoid(scores[:, width_neg : 2 * width_neg]) * (1.0 / width_neg)
        pos_coef = -jax.nn.sigmoid(-scores[:, 2 * width_neg :])
        pos_coef = pos_coef.astype(jnp.bfloat16).astype(jnp.float32)[:, :1]
        grads = s["grads"]
        grads[2 * group_len :] = (
            dot(jnp.transpose(tail_coef).astype(jnp.bfloat16), s["query"][...])
            + dot(jnp.transpose(head_coef).astype(jnp.bfloat16), s["probe"][...])
        ).astype(jnp.bfloat16)
        tail_coef = tail_coef.astype(jnp.bfloat16)
        head_coef = head_coef.astype(jnp.bfloat16)
        for block in range(blocks):
            cut = slice(block * lanes, (block + 1) * lanes)
            head = rows[:group_len, cut].astype(jnp.float32)
            tail = rows[group_len : 2 * group_len, cut].astype(jnp.float32)
            rel = spread_parts(rel_rows[group * group_len : (group + 1) * group_len, cut].astype(jnp.float32))
            noise = rows[2 * group_len :, cut]
            tail_pull = pos_coef * tail + dot(tail_coef, noise)
            head_pull = dot(head_coef, noise)
            head_side = pos_coef * head + head_pull
            grads[:group_len, cut] = times_conj(tail_pull, rel).astype(jnp.bfloat16)
            grads[group_len : 2 * group_len, cut] = times(head_side, rel).astype(jnp.bfloat16)
            rel_grad = times_conj(tail_pull, spread_parts(head)) + times_conj(tail, spread_parts(head_pull))
            span = slice(group * group_len, (group + 1) * group_len)
            if in_kernel_sum:
                per_tile = columns // near_size // lanes
                within = slice((block % per_tile) * lanes, (block % per_tile + 1) * lanes)
                s["tiles_out"][block // per_tile, span, within] = rel_grad.astype(jnp.bfloat16)
            else:
                rel_out[span, cut] = rel_grad.astype(jnp.bfloat16)

        @pl.loop(0, far_size)
        def _(index):
            there = lax.rem(far + line_step(index, far_size), far_size)
            at = place_row[group : group + 1] - there * merged
            picks = lax.broadcasted_iota(jnp.int32, (merged, request_count), 0) == at
            block = dot(one_hot(picks), grads[...]).astype(jnp.bfloat16)

            @pl.when(there == far)
            def _():
                s["give_in"][group, far] = block

            @pl.when(there != far)
            def _():
                s["give_out"][group, there] = block
                give_copy(group, there, far).start()

        if in_kernel_sum:
            s["tiles_in"][near, group * group_len : (group + 1) * group_len] = s["tiles_out"][
                near, group * group_len : (group + 1) * group_len
            ]
            for step in range(1, near_size):
                tiles_copy(group, step).start()

    def hand_copy(group, step, there):
        beside, peer = near_peer(step)
        return send(
            s["hand_out"].at[group, there, beside], s["hand_in"].at[group, near, there],
            s["hand_ss"].at[group, step, there], s["hand_rs"].at[group, step, there], peer,
        )

    def spread(group, index):
        there = lax.rem(far + index, far_size)

        @pl.when(index != 0)
        def _():
            give_copy(group, 0, there).wait_recv()

        targets = jnp.transpose(s["line_maps"][there])[:, group : group + 1]
        picks = lax.broadcasted_iota(jnp.int32, (near_size * slots, merged), 1) == targets
        rows = dot(one_hot(picks), s["give_in"][group, there]).astype(jnp.bfloat16)
        s["hand_out"][group, there] = rows.reshape(near_size, slots, columns)
        for step in range(1, near_size):
            hand_copy(group, step, there).start()
        s["hand_in"][group, near, there] = s["hand_out"][group, there, near]

    def add_up(group, step):
        beside = lax.rem(near + near_size - step, near_size)

        @pl.when(step != 0)
        def _():
            @pl.loop(0, far_size)
            def _(there):
                hand_copy(group, step, there).wait_recv()

        @pl.loop(0, far_size)
        def _(there):
            targets = s["own_ids"][beside, there][group : group + 1, :slots]
            hits = lax.broadcasted_iota(jnp.int32, (rows_here, slots), 0) == targets
            totals[...] += dot(one_hot(hits), s["hand_in"][group, beside, there])

    share_len = rel_count // far_size

    def share_copy(step):
        there, peer = line_peer(step)
        span = pl.ds(pl.multiple_of(there * share_len, share_len), share_len)
        return send(
            s["rel_part"].at[span], s["share_in"].at[far], s["share_ss"].at[step], s["share_rs"].at[step], peer
        )

    def rel_block(row, column):
        width = columns // near_size
        return rel_out.at[
            pl.ds(pl.multiple_of(row * share_len, share_len), share_len),
            pl.ds(pl.multiple_of(column * width, width), width),
        ]

    def line_gather(step, source):
        there, peer = line_peer(step)
        block = rel_block(source, near)
        return send(block, block, s["lg_ss"].at[step], s["lg_rs"].at[source], peer)

    def plane_gather(step, row, column):
        there, peer = near_peer(step)
        block = rel_block(row, column)
        return send(block, block, s["pg_ss"].at[step, row], s["pg_rs"].at[column, row], peer)

    def relation_parts():
        for step in range(1, near_size):
            rel_ids_copy(step).wait()
        for group in range(groups):
            for step in range(1, near_size):
                tiles_copy(group, step).wait_recv()
        chunk = 512 if rel_count % 512 == 0 else rel_count

        @pl.loop(0, rel_count // chunk)
        def _(index):
            first = index * chunk
            total = jnp.zeros((chunk, columns // near_size), jnp.float32)
            for beside in range(near_size):
                at = s["plane_rel"][beside][:1] - first
                hits = lax.broadcasted_iota(jnp.int32, (chunk, groups * group_len), 0) == at
                total += dot(one_hot(hits), s["tiles_in"][beside])
            s["rel_part"][pl.ds(pl.multiple_of(first, chunk), chunk)] = total.astype(jnp.bfloat16)

        for step in range(1, far_size):
            share_copy(step).start()

    def relation_share():
        total = s["rel_part"][pl.ds(pl.multiple_of(far * share_len, share_len), share_len)].astype(jnp.float32)
        for step in range(1, far_size):
            share_copy(step).wait_recv()
        for step in range(1, far_size):
            total += s["share_in"][lax.rem(far + step, far_size)].astype(jnp.float32)
        rel_block(far, near)[...] = total.astype(jnp.bfloat16)
        for step in range(1, far_size):
            line_gather(step, far).start()
        for step in range(1, near_size):
            plane_gather(step, far, near).start()

    def relation_forward():
        for step in range(1, far_size):
            row = lax.rem(far + step, far_size)
            line_gather(0, row).wait_recv()
            for beside in range(1, near_size):
                plane_gather(beside, row, near).start()

    def relation_end():
        for step in range(1, near_size):
            there, _ = near_peer(step)

            @pl.loop(0, far_size)
            def _(row):
                plane_gather(0, row, there).wait_recv()

    @pl.loop(0, far_size * near_size)
    def _(index):
        look_up(0, index)

    for group in range(1, groups):

        @pl.loop(0, far_size)
        def _(index):
            @pl.loop(0, near_size)
            def _(part):
                look_up(group, index * near_size + part)

            merge(group - 1, index)

    @pl.loop(0, far_size)
    def _(index):
        merge(groups - 1, index)

    totals[...] = jnp.zeros_like(totals)
    counts[...] = jnp.zeros_like(counts)

    @pl.loop(0, near_size)
    def _(beside):
        @pl.loop(0, far_size)
        def _(there):
            total = jnp.zeros((rows_here, 1), jnp.float32)
            for group in range(groups):
                targets = s["own_ids"][beside, there][group : group + 1, :slots]
                hits = lax.broadcasted_iota(jnp.int32, (rows_here, slots), 0) == targets
                total += jnp.sum(hits.astype(jnp.float32), axis=1, keepdims=True)
            counts[...] += total

    for group in range(groups):
        compute(group)
    for group in range(groups):

        @pl.loop(0, far_size)
        def _(index):
            spread(group, index)

        if in_kernel_sum and group == 0:
            relation_parts()

    if in_kernel_sum:
        relation_share()
    for group in range(groups):
        if in_kernel_sum and group == groups - 1:
            relation_forward()

        @pl.loop(0, near_size)
        def _(step):
            add_up(group, step)

    if in_kernel_sum:
        relation_end()

    for group in range(groups):
        for step in range(1, far_size):
            there = lax.rem(far + step, far_size)
            far_copy(group, there, 0).wait_send()
            give_copy(group, there, 0).wait_send()
        for step in range(1, parts):
            part_copy(group, step).wait_send()
        for step in range(1, near_size):

            @pl.loop(0, far_size)
            def _(there):
                near_copy(group, step, there).wait_send()
                hand_copy(group, step, there).wait_send()

    if in_kernel_sum:
        for step in range(1, near_size):
            for group in range(groups):
                tiles_copy(group, step).wait_send()

            @pl.loop(0, far_size)
            def _(row):
                plane_gather(step, row, near).wait_send()

        for step in range(1, far_size):
            share_copy(step).wait_send()
            line_gather(step, far).wait_send()


def exchange_step(inputs, sizes, collective_id):
    near_size, far_size, groups, slots, merged, group_len, width_neg, rel_count = sizes
    table, ids, maps = inputs[:3]
    rows_here, columns = table.shape
    parts = lax.axis_size("dim")
    dma = pltpu.SemaphoreType.DMA
    low = jnp.bfloat16
    vmem = pl.BlockSpec(memory_space=pltpu.VMEM)
    request_count = 2 * group_len + width_neg
    in_kernel_sum = columns % (2 * BLK * near_size) == 0
    scratch = {
        "line_ids": pltpu.VMEM(ids.shape, jnp.int32),
        "line_maps": pltpu.VMEM(maps.shape, jnp.int32),
        "own_ids": pltpu.VMEM((near_size, far_size) + ids.shape[2:], jnp.int32),
        "near_out": pltpu.VMEM((groups, near_size, far_size, slots, columns), low),
        "near_in": pltpu.VMEM((groups, far_size, near_size, slots, columns), low),
        "far_out": pltpu.VMEM((groups, far_size, merged, columns), low),
        "arrived": pltpu.VMEM((groups, far_size, merged, columns), low),
        "rows": pltpu.VMEM((request_count, columns), low),
        "grads": pltpu.VMEM((request_count, columns), low),
        "query": pltpu.VMEM((group_len, columns), low),
        "probe": pltpu.VMEM((group_len, columns), low),
        "part_all": pltpu.VMEM((groups, parts, group_len, 2 * width_neg + 128), low),
        "give_out": pltpu.VMEM((groups, far_size, merged, columns), low),
        "give_in": pltpu.VMEM((groups, far_size, merged, columns), low),
        "hand_out": pltpu.VMEM((groups, far_size, near_size, slots, columns), low),
        "hand_in": pltpu.VMEM((groups, near_size, far_size, slots, columns), low),
    }
    for name, shape in (
        ("ids", (far_size,)), ("maps", (far_size,)), ("fwd", (near_size,)),
        ("near", (groups, near_size, far_size)), ("far", (groups, far_size)),
        ("part", (groups, parts)), ("give", (groups, far_size)),
        ("hand", (groups, near_size, far_size)),
    ):
        scratch[name + "_ss"] = dma(shape)
        scratch[name + "_rs"] = dma(shape)
    if in_kernel_sum:
        width = columns // near_size
        scratch["plane_rel"] = pltpu.VMEM((near_size, 8, groups * group_len), jnp.int32)
        scratch["tiles_out"] = pltpu.VMEM((near_size, groups * group_len, width), low)
        scratch["tiles_in"] = pltpu.VMEM((near_size, groups * group_len, width), low)
        scratch["rel_part"] = pltpu.VMEM((rel_count, width), low)
        scratch["share_in"] = pltpu.VMEM((far_size, rel_count // far_size, width), low)
        for name, shape in (
            ("rid", (near_size,)), ("tiles", (groups, near_size)), ("share", (far_size,)),
            ("lg", (far_size,)), ("pg", (near_size, far_size)),
        ):
            scratch[name + "_ss"] = dma(shape)
            scratch[name + "_rs"] = dma(shape)
    names = tuple(scratch)
    rel_rows_out = rel_count if in_kernel_sum else groups * group_len

    def kernel(*refs):
        step_kernel(sizes, refs[:7], refs[7:10], dict(zip(names, refs[10:])))

    return pl.pallas_call(
        kernel,
        name="exchange_step",
        out_shape=(
            jax.ShapeDtypeStruct((rows_here, columns), jnp.float32),
            jax.ShapeDtypeStruct((rows_here, 1), jnp.float32),
            jax.ShapeDtypeStruct((rel_rows_out, columns), low),
        ),
        in_specs=[vmem] * 7,
        out_specs=(vmem,) * 3,
        scratch_shapes=list(scratch.values()),
        compiler_params=pltpu.CompilerParams(
            collective_id=collective_id, has_side_effects=True, vmem_limit_bytes=VMEM_LIMIT
        ),
    )(*inputs)


def placement_of(wanted_row, rows_here, sizes):
    near_size, far_size, slots = sizes
    owners = near_size * far_size
    request_count = wanted_row.shape[0]
    owner_of = wanted_row // rows_here
    owner_hits = (owner_of[:, None] == jnp.arange(owners, dtype=jnp.int32)[None, :]).astype(
        jnp.bfloat16
    )
    order = jnp.arange(request_count, dtype=jnp.int32)
    earlier = (order[:, None] > order[None, :]).astype(jnp.bfloat16)
    before = jnp.dot(earlier, owner_hits, preferred_element_type=jnp.float32)
    slot_rank = jnp.sum(before * owner_hits.astype(jnp.float32), axis=-1).astype(jnp.int32)
    plane_of = owner_of // near_size
    same_plane = (
        plane_of[:, None] == (jnp.arange(owners, dtype=jnp.int32) // near_size)[None, :]
    ).astype(jnp.float32)
    plane_rank = jnp.sum(before * same_plane, axis=-1).astype(jnp.int32)
    slot_flat = owner_of * slots + slot_rank
    at_slot = slot_flat[:, None] == jnp.arange(owners * slots, dtype=jnp.int32)[None, :]
    local_row = wanted_row - owner_of * rows_here
    slot_ids = jnp.sum(jnp.where(at_slot, local_row[:, None] + 1, 0), axis=0) - 1
    slot_map = jnp.sum(jnp.where(at_slot, plane_rank[:, None] + 1, 0), axis=0) - 1
    return (plane_of, plane_rank, slot_ids, slot_map)


def teams(near_size, far_size):
    near = [[row * near_size + place for place in range(near_size)] for row in range(far_size)]
    far = [[row * near_size + place for row in range(far_size)] for place in range(near_size)]
    return (near, far)


def sum_relations(rel_rows, near_ids, rel_count, near, far):
    near_size, far_size = len(far), len(near)
    row_count, columns = rel_rows.shape
    tiles = rel_rows.reshape(row_count, near_size, columns // near_size).transpose(1, 0, 2)
    tiles = lax.all_to_all(
        tiles, "ent", split_axis=0, concat_axis=0, axis_index_groups=near, tiled=True
    )
    hits = (near_ids[:, None] == jnp.arange(rel_count, dtype=jnp.int32)[None, :]).astype(
        jnp.bfloat16
    )
    part = contract_first(hits, tiles.reshape(near_size * row_count, columns // near_size)).astype(
        jnp.bfloat16
    )
    share = lax.psum_scatter(
        part, "ent", scatter_dimension=0, axis_index_groups=far, tiled=True
    )
    whole = lax.all_gather(share, "ent", axis=0)
    whole = whole.reshape(far_size, near_size, rel_count // far_size, columns // near_size)
    return whole.transpose(0, 2, 1, 3).reshape(rel_count, columns)


def adagrad(table, state, grad, squares):
    new_state = state + squares / (2 * RANK)
    scale = LEARN_RATE / jnp.sqrt(new_state)
    return table - grad * scale[:, None]


def per_device(entities, ent_state, buckets, relations, rel_state, triples, negatives):
    owners = lax.axis_size("ent")
    rows_here, columns_here = entities.shape
    rel_count = relations.shape[0]
    groups_here, width_neg = negatives.shape
    group_len = triples.shape[1] // groups_here
    request_count = 2 * group_len + width_neg
    slots = 8 * ((request_count + 3 * owners - 1) // (3 * owners))
    near_size = 4 if owners % 4 == 0 else 1
    far_size = owners // near_size
    most = min(near_size * slots, request_count)
    few = min(most, 16 * ((19 * slots + 127) // 128))
    ent_low = entities.astype(jnp.bfloat16)
    head_ids = triples[0].reshape(groups_here, group_len)
    tail_ids = triples[2].reshape(groups_here, group_len)
    wanted = jnp.concatenate([head_ids, tail_ids, negatives], axis=1)
    placed = [
        placement_of(wanted[index], rows_here, (near_size, far_size, slots))
        for index in range(groups_here)
    ]
    plane_of = jnp.stack([each[0] for each in placed])
    plane_rank = jnp.stack([each[1] for each in placed])
    longest = lax.pmax(jnp.max(plane_rank) + 1, ("ent", "dim"))
    slot_ids = jnp.stack([each[2] for each in placed])
    slot_ids = slot_ids.reshape(groups_here, far_size, near_size, slots).transpose(1, 2, 0, 3)
    slot_ids = jnp.pad(
        slot_ids, ((0, 0), (0, 0), (0, 8 - groups_here), (0, 128 - slots)), constant_values=-1
    )
    slot_maps = jnp.stack([each[3] for each in placed])
    slot_maps = slot_maps.reshape(groups_here, far_size, near_size * slots).transpose(1, 0, 2)
    slot_maps = jnp.pad(slot_maps, ((0, 0), (0, 8 - groups_here), (0, 0)), constant_values=-1)
    rel_rows = jnp.take(relations, triples[1], axis=0, mode="clip").astype(jnp.bfloat16)
    rel_ids = jnp.broadcast_to(triples[1][None, :], (8, triples.shape[1]))

    def run(merged, collective_id):
        def branch(plane_of, plane_rank, *inputs):
            place = plane_of * merged + plane_rank
            place_row = jnp.pad(place, ((0, 8 - groups_here), (0, 0)), constant_values=-1)
            sizes = (near_size, far_size, groups_here, slots, merged, group_len, width_neg, rel_count)
            table, ids, maps, rel_rows, rel_ids = inputs
            return exchange_step(
                (table, ids, maps, place_row.T, place_row, rel_rows, rel_ids), sizes, collective_id
            )

        return branch

    operands = (plane_of, plane_rank, ent_low, slot_ids, slot_maps, rel_rows, rel_ids)
    totals, counts, rel_grad = lax.cond(longest <= few, run(few, 0), run(most, 1), *operands)
    if rel_grad.shape[0] != rel_count:
        near, far = teams(near_size, far_size)
        near_ids = lax.all_gather(triples[1], "ent", axis_index_groups=near, tiled=True)
        rel_grad = sum_relations(rel_grad, near_ids, rel_count, near, far)
    rel_grad = rel_grad.astype(jnp.float32)
    weight = REG_WEIGHT * (buckets.astype(jnp.float32) + 1.0) * counts[:, 0]
    totals = totals + weight[:, None] * 3.0 * entities * jnp.abs(entities)
    ent_squares = jnp.sum(totals * totals, axis=-1)
    ent_all, rel_all = lax.psum((ent_squares, jnp.sum(rel_grad * rel_grad, axis=-1)), "dim")
    new_relations = adagrad(relations, rel_state, rel_grad, rel_all)
    new_entities = adagrad(entities, ent_state, totals, ent_all)
    return (new_entities, new_relations)


def solution(mesh):
    placed = (
        P("ent", "dim"),
        P("ent"),
        P("ent"),
        P(None, "dim"),
        P(),
        P(None, "ent"),
        P("ent", None),
    )
    return jax.shard_map(
        per_device,
        mesh=mesh,
        in_specs=placed,
        out_specs=(P("ent", "dim"), P(None, "dim")),
        check_vma=False,
    )
```

```python
import functools

import jax
import jax.numpy as jnp
from jax import lax
from jax.experimental import pallas as pl
from jax.experimental.pallas import tpu as pltpu
from jax.sharding import PartitionSpec as P

RANK = 512
BLK = 64


LEARN_RATE = 0.1
REG_WEIGHT = 0.01
MESH = pl.DeviceIdType.MESH
VMEM_LIMIT = 60 * 1024 * 1024


def contract_first(former, latter):
    return lax.dot_general(
        former, latter, (((0,), (0,)), ((), ())), preferred_element_type=jnp.float32
    )


def contract_last(former, latter):
    return lax.dot_general(
        former, latter, (((1,), (1,)), ((), ())), preferred_element_type=jnp.float32
    )


def position(near_size):
    me = lax.axis_index("ent")
    return lax.div(me, near_size), lax.rem(me, near_size)


def greet(near_size, far_size, with_parts=True):
    far, near = position(near_size)
    parts = lax.axis_size("dim") if with_parts else 1
    barrier = pltpu.get_barrier_semaphore()
    for step in range(1, parts):
        peer = lax.rem(lax.axis_index("dim") + step, parts)
        pl.semaphore_signal(barrier, inc=1, device_id={"dim": peer}, device_id_type=MESH)
    for step in range(1, near_size):
        peer = far * near_size + lax.rem(near + step, near_size)
        pl.semaphore_signal(barrier, inc=1, device_id={"ent": peer}, device_id_type=MESH)
    for step in range(1, far_size):
        peer = lax.rem(far + step, far_size) * near_size + near
        pl.semaphore_signal(barrier, inc=1, device_id={"ent": peer}, device_id_type=MESH)
    pl.semaphore_wait(barrier, near_size + far_size + parts - 3)


def send(source, target, send_sem, recv_sem, peer, axis="ent"):
    return pltpu.make_async_remote_copy(
        src_ref=source,
        dst_ref=target,
        send_sem=send_sem,
        recv_sem=recv_sem,
        device_id={axis: peer},
        device_id_type=MESH,
    )


def line_step(index, far_size):
    return jnp.where(
        index == far_size - 1, 0, 1 + lax.rem(far_size // 2 - 1 + index, far_size - 1)
    )


def one_hot(condition):
    return condition.astype(jnp.float32).astype(jnp.bfloat16)


def dot(former, latter):
    return jnp.dot(former, latter, preferred_element_type=jnp.float32)


def swapped(values):
    return pltpu.roll(values, BLK, 1)


def spread_parts(values):
    other = swapped(values)
    first = lax.broadcasted_iota(jnp.int32, values.shape, 1) < BLK
    return jnp.where(first, values, other), jnp.where(first, -other, values)


def times(former, parts):
    return former * parts[0] + swapped(former) * parts[1]


def times_conj(former, parts):
    return former * parts[0] - swapped(former) * parts[1]


def ids_kernel(sizes, ids, maps, rel_ids, own_ids, line_maps, plane_rel, line_ids, *sems):
    near_size, far_size = sizes
    ids_ss, ids_rs, maps_ss, maps_rs, fwd_ss, fwd_rs, rid_ss, rid_rs = sems
    far, near = position(near_size)
    greet(near_size, far_size, False)

    def line_peer(step):
        there = lax.rem(far + step, far_size)
        return there, there * near_size + near

    def near_peer(step):
        there = lax.rem(near + step, near_size)
        return there, far * near_size + there

    def ids_copy(step):
        there, peer = line_peer(step)
        return send(ids.at[there], line_ids.at[far], ids_ss.at[step], ids_rs.at[step], peer)

    def maps_copy(step):
        there, peer = line_peer(step)
        return send(maps.at[there], line_maps.at[far], maps_ss.at[step], maps_rs.at[step], peer)

    def fwd_copy(step):
        there, peer = near_peer(step)
        return send(line_ids.at[:, there], own_ids.at[near], fwd_ss.at[step], fwd_rs.at[step], peer)

    def rel_ids_copy(step):
        there, peer = near_peer(step)
        return send(rel_ids, plane_rel.at[near], rid_ss.at[step], rid_rs.at[step], peer)

    for step in range(1, far_size):
        ids_copy(step).start()
    for step in range(1, far_size):
        maps_copy(step).start()
    for step in range(1, near_size):
        rel_ids_copy(step).start()
    plane_rel[near] = rel_ids[...]
    line_ids[far] = ids[far]
    line_maps[far] = maps[far]
    for step in range(1, far_size):
        ids_copy(step).wait()
    longest = line_ids[0, 0, 7:8]
    for there in range(1, far_size):
        longest = jnp.maximum(longest, line_ids[there, 0, 7:8])
    for there in range(far_size):
        for beside in range(near_size):
            line_ids[there, beside, 7:8] = longest
    for step in range(1, near_size):
        fwd_copy(step).start()
    own_ids[near] = line_ids[:, near]
    for step in range(1, near_size):
        fwd_copy(step).wait()
    for step in range(1, far_size):
        maps_copy(step).wait()
    for step in range(1, near_size):
        rel_ids_copy(step).wait()


def share_ids(ids, maps, rel_ids, sizes):
    near_size, far_size = sizes
    dma = pltpu.SemaphoreType.DMA
    vmem = pl.BlockSpec(memory_space=pltpu.VMEM)
    return pl.pallas_call(
        functools.partial(ids_kernel, sizes),
        name="share_ids",
        out_shape=(
            jax.ShapeDtypeStruct((near_size, far_size) + ids.shape[2:], jnp.int32),
            jax.ShapeDtypeStruct(maps.shape, jnp.int32),
            jax.ShapeDtypeStruct((near_size,) + rel_ids.shape, jnp.int32),
        ),
        in_specs=[vmem] * 3,
        out_specs=(vmem,) * 3,
        scratch_shapes=[pltpu.VMEM(ids.shape, jnp.int32)]
        + [dma((far_size,))] * 4
        + [dma((near_size,))] * 4,
        compiler_params=pltpu.CompilerParams(collective_id=2, has_side_effects=True),
    )(ids, maps, rel_ids)


def step_kernel(sizes, refs_in, refs_out, scratch):
    near_size, far_size, groups, slots, merged, group_len, width_neg, rel_count = sizes
    table, own_ids, line_maps, place, rel_rows, plane_rel = refs_in
    totals, counts, rel_out = refs_out
    s = scratch
    rows_here, columns = table.shape
    in_kernel_sum = "tiles_in" in s
    far, near = position(near_size)
    parts = lax.axis_size("dim")
    part_here = lax.axis_index("dim")
    greet(near_size, far_size)

    def line_peer(step):
        there = lax.rem(far + step, far_size)
        return there, there * near_size + near

    def near_peer(step):
        there = lax.rem(near + step, near_size)
        return there, far * near_size + there

    def near_copy(group, step, there):
        beside, peer = near_peer(step)
        return send(
            s["near_out"].at[group, step, there], s["near_in"].at[group, there, near],
            s["near_ss"].at[group, step, there], s["near_rs"].at[group, step, there], peer,
        )

    def look_up(group, index):
        step = lax.rem(index + 1, near_size)
        there = lax.rem(far + line_step(lax.div(index, near_size), far_size), far_size)
        beside = lax.rem(near + step, near_size)
        wanted = jnp.transpose(own_ids[beside, there])[:slots, group : group + 1]
        hits = wanted == lax.broadcasted_iota(jnp.int32, (slots, rows_here), 1)
        found = dot(one_hot(hits), table[...]).astype(jnp.bfloat16)

        @pl.when(step == 0)
        def _():
            s["near_in"][group, there, near] = found

        @pl.when(step != 0)
        def _():
            s["near_out"][group, step, there] = found
            near_copy(group, step, there).start()

    def far_copy(group, there, source):
        return send(
            s["far_out"].at[group, there], s["arrived"].at[group, source],
            s["far_ss"].at[group, there], s["far_rs"].at[group, source], there * near_size + near,
        )

    def merge(group, index):
        there = lax.rem(far + line_step(index, far_size), far_size)
        for step in range(1, near_size):
            near_copy(group, step, there).wait_recv()
        targets = line_maps[there][group : group + 1]
        picks = lax.broadcasted_iota(jnp.int32, (merged, near_size * slots), 0) == targets
        rows = s["near_in"][group, there].reshape(near_size * slots, columns)
        block = dot(one_hot(picks), rows).astype(jnp.bfloat16)

        @pl.when(there == far)
        def _():
            s["arrived"][group, far] = block

        @pl.when(there != far)
        def _():
            s["far_out"][group, there] = block
            far_copy(group, there, far).start()

    def part_copy(group, step):
        peer = lax.rem(part_here + step, parts)
        return send(
            s["part_all"].at[group, part_here], s["part_all"].at[group, part_here],
            s["part_ss"].at[group, step], s["part_rs"].at[group, step], peer, axis="dim",
        )

    def tiles_copy(group, step):
        there, peer = near_peer(step)
        span = pl.ds(group * group_len, group_len)
        return send(
            s["tiles_out"].at[there, span], s["tiles_in"].at[near, span],
            s["tiles_ss"].at[group, step], s["tiles_rs"].at[group, step], peer,
        )

    def give_copy(group, there, source):
        return send(
            s["give_out"].at[group, there], s["give_in"].at[group, source],
            s["give_ss"].at[group, there], s["give_rs"].at[group, source], there * near_size + near,
        )

    lanes = 2 * BLK
    blocks = columns // lanes

    def compute(group):
        for step in range(1, far_size):
            far_copy(group, 0, lax.rem(far + step, far_size)).wait_recv()
        place_col = jnp.transpose(place[:8])
        place_col = place_col[:, :groups] * merged + place_col[:, groups : 2 * groups]
        incoming = s["arrived"][group].reshape(far_size * merged, columns)
        request_count = 2 * group_len + width_neg
        rows = s["rows"]
        third = 256 if request_count % 256 == 0 else request_count
        for start in range(0, request_count, third):
            at = place_col[start : start + third, group : group + 1]
            picks = lax.broadcasted_iota(jnp.int32, (third, far_size * merged), 1) == at
            rows[start : start + third] = dot(one_hot(picks), incoming).astype(jnp.bfloat16)
        pos = jnp.zeros((group_len, 1), jnp.float32)
        for block in range(blocks):
            cut = slice(block * lanes, (block + 1) * lanes)
            head = rows[:group_len, cut].astype(jnp.float32)
            tail = rows[group_len : 2 * group_len, cut].astype(jnp.float32)
            rel = spread_parts(rel_rows[group * group_len : (group + 1) * group_len, cut].astype(jnp.float32))
            query = times(head, rel).astype(jnp.bfloat16)
            s["query"][:, cut] = query
            s["probe"][:, cut] = times_conj(tail, rel).astype(jnp.bfloat16)
            pos += jnp.sum(query.astype(jnp.float32) * tail, axis=1, keepdims=True)
        noise = rows[2 * group_len :]
        part = s["part_all"]
        part[group, part_here, :, :width_neg] = contract_last(s["query"][...], noise).astype(jnp.bfloat16)
        part[group, part_here, :, width_neg : 2 * width_neg] = contract_last(
            s["probe"][...], noise
        ).astype(jnp.bfloat16)
        part[group, part_here, :, 2 * width_neg :] = jnp.broadcast_to(pos, (group_len, 128)).astype(
            jnp.bfloat16
        )
        for step in range(1, parts):
            part_copy(group, step).start()
        for step in range(1, parts):
            part_copy(group, step).wait_recv()
        scores = part[group, 0].astype(jnp.float32)
        for other in range(1, parts):
            scores += part[group, other].astype(jnp.float32)
        tail_coef = jax.nn.sigmoid(scores[:, :width_neg]) * (1.0 / width_neg)
        head_coef = jax.nn.sigmoid(scores[:, width_neg : 2 * width_neg]) * (1.0 / width_neg)
        pos_coef = -jax.nn.sigmoid(-scores[:, 2 * width_neg :])
        pos_coef = pos_coef.astype(jnp.bfloat16).astype(jnp.float32)[:, :1]
        grads = s["grads"]
        grads[2 * group_len :] = (
            dot(jnp.transpose(tail_coef).astype(jnp.bfloat16), s["query"][...])
            + dot(jnp.transpose(head_coef).astype(jnp.bfloat16), s["probe"][...])
        ).astype(jnp.bfloat16)
        tail_coef = tail_coef.astype(jnp.bfloat16)
        head_coef = head_coef.astype(jnp.bfloat16)
        for block in range(blocks):
            cut = slice(block * lanes, (block + 1) * lanes)
            head = rows[:group_len, cut].astype(jnp.float32)
            tail = rows[group_len : 2 * group_len, cut].astype(jnp.float32)
            rel = spread_parts(rel_rows[group * group_len : (group + 1) * group_len, cut].astype(jnp.float32))
            noise = rows[2 * group_len :, cut]
            tail_pull = pos_coef * tail + dot(tail_coef, noise)
            head_pull = dot(head_coef, noise)
            head_side = pos_coef * head + head_pull
            grads[:group_len, cut] = times_conj(tail_pull, rel).astype(jnp.bfloat16)
            grads[group_len : 2 * group_len, cut] = times(head_side, rel).astype(jnp.bfloat16)
            rel_grad = times_conj(tail_pull, spread_parts(head)) + times_conj(tail, spread_parts(head_pull))
            span = slice(group * group_len, (group + 1) * group_len)
            if in_kernel_sum:
                per_tile = columns // near_size // lanes
                within = slice((block % per_tile) * lanes, (block % per_tile + 1) * lanes)
                s["tiles_out"][block // per_tile, span, within] = rel_grad.astype(jnp.bfloat16)
            else:
                rel_out[span, cut] = rel_grad.astype(jnp.bfloat16)

        if in_kernel_sum:
            s["tiles_in"][near, group * group_len : (group + 1) * group_len] = s["tiles_out"][
                near, group * group_len : (group + 1) * group_len
            ]
            for step in range(1, near_size):
                tiles_copy(group, step).start()

    def give_blocks(group):
        @pl.loop(0, far_size)
        def _(index):
            there = lax.rem(far + line_step(index, far_size), far_size)
            at = place[groups + group : groups + group + 1] + (place[group : group + 1] - there) * merged
            picks = lax.broadcasted_iota(jnp.int32, (merged, s["grads"].shape[0]), 0) == at
            block = dot(one_hot(picks), s["grads"][...]).astype(jnp.bfloat16)

            @pl.when(there == far)
            def _():
                s["give_in"][group, far] = block

            @pl.when(there != far)
            def _():
                s["give_out"][group, there] = block

    def give_start(group, index):
        there = lax.rem(far + line_step(index, far_size), far_size)
        give_copy(group, there, far).start()

    def hand_copy(group, step, there):
        beside, peer = near_peer(step)
        return send(
            s["hand_out"].at[group, there, beside], s["hand_in"].at[group, near, there],
            s["hand_ss"].at[group, step, there], s["hand_rs"].at[group, step, there], peer,
        )

    def spread(group, index):
        offset = jnp.where(index == 0, 0, far_size - line_step(index - 1, far_size))
        there = lax.rem(far + offset, far_size)

        @pl.when(index != 0)
        def _():
            give_copy(group, 0, there).wait_recv()

        targets = jnp.transpose(line_maps[there])[:, group : group + 1]
        picks = lax.broadcasted_iota(jnp.int32, (near_size * slots, merged), 1) == targets
        rows = dot(one_hot(picks), s["give_in"][group, there]).astype(jnp.bfloat16)
        s["hand_out"][group, there] = rows.reshape(near_size, slots, columns)
        for step in range(1, near_size):
            hand_copy(group, step, there).start()
        s["hand_in"][group, near, there] = s["hand_out"][group, there, near]

    def add_up(group, step):
        beside = lax.rem(near + near_size - step, near_size)

        @pl.when(step != 0)
        def _():
            @pl.loop(0, far_size)
            def _(there):
                hand_copy(group, step, there).wait_recv()

        @pl.loop(0, far_size)
        def _(there):
            targets = own_ids[beside, there][group : group + 1, :slots]
            hits = lax.broadcasted_iota(jnp.int32, (rows_here, slots), 0) == targets
            totals[...] += dot(one_hot(hits), s["hand_in"][group, beside, there])

    def add_up_all(group):
        @pl.loop(0, near_size)
        def _(step):
            add_up(group, step)

    share_len = rel_count // far_size
    beside_far = far + 1 - 2 * lax.rem(far, 2)
    across_far = lax.rem(far + 2, 4)
    diagonal_far = lax.rem(beside_far + 2, 4)
    line = lambda there: there * near_size + near
    near_x = near + 1 - 2 * lax.rem(near, 2)
    near_y = lax.rem(near + 2, 4)
    near_xy = lax.rem(near_x + 2, 4)
    plane = lambda there: far * near_size + there

    def share_rows(row):
        return pl.ds(pl.multiple_of(row * share_len, share_len), share_len)

    def halve_copy(index):
        row = beside_far if index == 0 else diagonal_far
        return send(
            s["rel_part"].at[share_rows(row)], s["share_in"].at[index],
            s["halve_ss"].at[index], s["halve_rs"].at[index], line(beside_far),
        )

    def across_copy():
        return send(
            s["share_out"], s["share_in"].at[2], s["double_ss"].at[2], s["double_rs"].at[2], line(across_far)
        )

    def rel_block(row, column, half=None):
        width = columns // near_size
        start = row * share_len
        length = share_len
        if half is not None:
            length = share_len // 2
            start = start + half * length
        return rel_out.at[
            pl.ds(pl.multiple_of(start, length), length),
            pl.ds(pl.multiple_of(column * width, width), width),
        ]

    known_rows = (far, across_far, beside_far, diagonal_far)

    def double_copy(index, row):
        peer = across_far if index == 0 else beside_far
        block = rel_block(row, near)
        return send(block, block, s["double_ss"].at[index], s["double_rs"].at[index], line(peer))

    def pass_copy(row):
        block = rel_block(row, near)
        return send(block, block, s["pass_ss"].at[0], s["pass_rs"].at[0], line(beside_far))

    def plane_copy(way, row, column):
        peer = near_x if way == 0 else near_y
        block = rel_block(row, column)
        return send(block, block, s["pg_ss"].at[way, row], s["pg_rs"].at[way, row], plane(peer))

    def relay_copy(way, row, column):
        peer = near_y if way == 0 else near_x
        block = rel_block(row, column, way)
        return send(block, block, s["relay_ss"].at[way, row], s["relay_rs"].at[way, row], plane(peer))

    def relation_parts():
        for group in range(groups):
            for step in range(1, near_size):
                tiles_copy(group, step).wait_recv()
        chunk = 512 if rel_count % 512 == 0 else rel_count

        @pl.loop(0, rel_count // chunk)
        def _(index):
            first = index * chunk
            total = jnp.zeros((chunk, columns // near_size), jnp.float32)
            for beside in range(near_size):
                at = plane_rel[beside][:1] - first
                hits = lax.broadcasted_iota(jnp.int32, (chunk, groups * group_len), 0) == at
                total += dot(one_hot(hits), s["tiles_in"][beside])
            s["rel_part"][pl.ds(pl.multiple_of(first, chunk), chunk)] = total.astype(jnp.bfloat16)

        for index in range(2):
            halve_copy(index).start()

    def part_rows(row):
        return s["rel_part"][share_rows(row)].astype(jnp.float32)

    def relation_across():
        halve_copy(1).wait_recv()
        s["share_out"][...] = (part_rows(across_far) + s["share_in"][1].astype(jnp.float32)).astype(jnp.bfloat16)
        across_copy().start()

    def relation_share():
        halve_copy(0).wait_recv()
        total = part_rows(far) + s["share_in"][0].astype(jnp.float32)
        across_copy().wait_recv()
        total += s["share_in"][2].astype(jnp.float32)
        rel_block(far, near)[...] = total.astype(jnp.bfloat16)
        double_copy(0, far).start()
        double_copy(1, far).start()
        for way in range(2):
            plane_copy(way, far, near).start()

    def relation_known(row):
        for way in range(2):
            plane_copy(way, row, near).start()

    def relation_relay(row):
        plane_copy(0, row, near_x).wait_recv()
        relay_copy(0, row, near_x).start()
        plane_copy(1, row, near_y).wait_recv()
        relay_copy(1, row, near_y).start()

    def relation_end():
        for row in known_rows:
            for way in range(2):
                relay_copy(way, row, near_xy).wait_recv()

    def count_part(beside):
        @pl.loop(0, far_size)
        def _(there):
            total = jnp.zeros((rows_here, 1), jnp.float32)
            for group in range(groups):
                targets = own_ids[beside, there][group : group + 1, :slots]
                hits = lax.broadcasted_iota(jnp.int32, (rows_here, slots), 0) == targets
                total += jnp.sum(hits.astype(jnp.float32), axis=1, keepdims=True)
            counts[...] += total

    @pl.loop(0, far_size * near_size)
    def _(index):
        look_up(0, index)

    for group in range(1, groups):

        @pl.loop(0, far_size)
        def _(index):
            @pl.loop(0, near_size)
            def _(part):
                look_up(group, index * near_size + part)

            merge(group - 1, index)

    totals[...] = jnp.zeros_like(totals)
    counts[...] = jnp.zeros_like(counts)

    @pl.loop(0, near_size)
    def _(beside):
        count_part(beside)

    last = groups - 1
    early = far_size // 2 if groups > 1 else far_size

    @pl.loop(0, early)
    def _(index):
        merge(last, index)

    for group in range(last):
        compute(group)
        if group == 0:

            @pl.loop(early, far_size)
            def _(index):
                merge(last, index)

        give_blocks(group)
        for index in range(far_size - 1):
            give_start(group, index)

    compute(last)
    give_blocks(last)
    if in_kernel_sum:
        relation_parts()
        give_start(last, 0)
        for group in range(last):

            @pl.loop(0, far_size)
            def _(index):
                spread(group, index)

        relation_across()
        give_start(last, 1)
        relation_share()
        give_start(last, 2)
        for group in range(last):
            add_up_all(group)
        spread(last, 0)
        double_copy(0, across_far).wait_recv()
        pass_copy(across_far).start()
        relation_known(across_far)
        relation_relay(far)
        double_copy(1, beside_far).wait_recv()
        relation_known(beside_far)
        spread(last, 1)
        pass_copy(diagonal_far).wait_recv()
        relation_known(diagonal_far)
        relation_relay(across_far)
        relation_relay(beside_far)
        spread(last, 2)
        spread(last, 3)
        relation_relay(diagonal_far)
        add_up_all(last)
        relation_end()
    else:
        for index in range(far_size - 1):
            give_start(last, index)
        for group in range(groups):

            @pl.loop(0, far_size)
            def _(index):
                spread(group, index)

        for group in range(groups):
            add_up_all(group)

    for group in range(groups):
        for step in range(1, far_size):
            there = lax.rem(far + step, far_size)
            far_copy(group, there, 0).wait_send()
            give_copy(group, there, 0).wait_send()
        for step in range(1, parts):
            part_copy(group, step).wait_send()
        for step in range(1, near_size):

            @pl.loop(0, far_size)
            def _(there):
                near_copy(group, step, there).wait_send()
                hand_copy(group, step, there).wait_send()

    if in_kernel_sum:
        for step in range(1, near_size):
            for group in range(groups):
                tiles_copy(group, step).wait_send()
        for index in range(2):
            halve_copy(index).wait_send()
            double_copy(index, far).wait_send()
        across_copy().wait_send()
        pass_copy(across_far).wait_send()
        for row in known_rows:
            for way in range(2):
                plane_copy(way, row, near).wait_send()
                relay_copy(way, row, near).wait_send()


def sums_in_kernel(columns, near_size, far_size):
    return near_size == 4 and far_size == 4 and columns % (2 * BLK * near_size) == 0


def exchange_step(inputs, sizes, collective_id):
    near_size, far_size, groups, slots, merged, group_len, width_neg, rel_count = sizes
    table = inputs[0]
    rows_here, columns = table.shape
    parts = lax.axis_size("dim")
    dma = pltpu.SemaphoreType.DMA
    low = jnp.bfloat16
    vmem = pl.BlockSpec(memory_space=pltpu.VMEM)
    request_count = 2 * group_len + width_neg
    in_kernel_sum = sums_in_kernel(columns, near_size, far_size)
    scratch = {
        "near_out": pltpu.VMEM((groups, near_size, far_size, slots, columns), low),
        "near_in": pltpu.VMEM((groups, far_size, near_size, slots, columns), low),
        "far_out": pltpu.VMEM((groups, far_size, merged, columns), low),
        "arrived": pltpu.VMEM((groups, far_size, merged, columns), low),
        "rows": pltpu.VMEM((request_count, columns), low),
        "grads": pltpu.VMEM((request_count, columns), low),
        "query": pltpu.VMEM((group_len, columns), low),
        "probe": pltpu.VMEM((group_len, columns), low),
        "part_all": pltpu.VMEM((groups, parts, group_len, 2 * width_neg + 128), low),
        "give_out": pltpu.VMEM((groups, far_size, merged, columns), low),
        "give_in": pltpu.VMEM((groups, far_size, merged, columns), low),
        "hand_out": pltpu.VMEM((groups, far_size, near_size, slots, columns), low),
        "hand_in": pltpu.VMEM((groups, near_size, far_size, slots, columns), low),
    }
    for name, shape in (
        ("near", (groups, near_size, far_size)), ("far", (groups, far_size)),
        ("part", (groups, parts)), ("give", (groups, far_size)),
        ("hand", (groups, near_size, far_size)),
    ):
        scratch[name + "_ss"] = dma(shape)
        scratch[name + "_rs"] = dma(shape)
    if in_kernel_sum:
        width = columns // near_size
        scratch["tiles_out"] = pltpu.VMEM((near_size, groups * group_len, width), low)
        scratch["tiles_in"] = pltpu.VMEM((near_size, groups * group_len, width), low)
        scratch["rel_part"] = pltpu.VMEM((rel_count, width), low)
        scratch["share_in"] = pltpu.VMEM((3, rel_count // far_size, width), low)
        scratch["share_out"] = pltpu.VMEM((rel_count // far_size, width), low)
        for name, shape in (
            ("tiles", (groups, near_size)), ("halve", (2,)), ("double", (3,)), ("pass", (1,)),
            ("pg", (2, far_size)), ("relay", (2, far_size)),
        ):
            scratch[name + "_ss"] = dma(shape)
            scratch[name + "_rs"] = dma(shape)
    names = tuple(scratch)
    rel_rows_out = rel_count if in_kernel_sum else groups * group_len

    def kernel(*refs):
        step_kernel(sizes, refs[:6], refs[6:9], dict(zip(names, refs[9:])))

    return pl.pallas_call(
        kernel,
        name="exchange_step",
        out_shape=(
            jax.ShapeDtypeStruct((rows_here, columns), jnp.float32),
            jax.ShapeDtypeStruct((rows_here, 1), jnp.float32),
            jax.ShapeDtypeStruct((rel_rows_out, columns), low),
        ),
        in_specs=[vmem] * 6,
        out_specs=(vmem,) * 3,
        scratch_shapes=list(scratch.values()),
        compiler_params=pltpu.CompilerParams(
            collective_id=collective_id, has_side_effects=True, vmem_limit_bytes=VMEM_LIMIT
        ),
    )(*inputs)


def placement_of(wanted_row, rows_here, sizes):
    near_size, far_size, slots = sizes
    owners = near_size * far_size
    request_count = wanted_row.shape[0]
    owner_of = wanted_row // rows_here
    owner_hits = (owner_of[:, None] == jnp.arange(owners, dtype=jnp.int32)[None, :]).astype(
        jnp.bfloat16
    )
    order = jnp.arange(request_count, dtype=jnp.int32)
    earlier = (order[:, None] > order[None, :]).astype(jnp.bfloat16)
    before = jnp.dot(earlier, owner_hits, preferred_element_type=jnp.float32)
    slot_rank = jnp.sum(before * owner_hits.astype(jnp.float32), axis=-1).astype(jnp.int32)
    plane_of = owner_of // near_size
    same_plane = (
        plane_of[:, None] == (jnp.arange(owners, dtype=jnp.int32) // near_size)[None, :]
    ).astype(jnp.float32)
    plane_rank = jnp.sum(before * same_plane, axis=-1).astype(jnp.int32)
    slot_flat = owner_of * slots + slot_rank
    at_slot = slot_flat[:, None] == jnp.arange(owners * slots, dtype=jnp.int32)[None, :]
    local_row = wanted_row - owner_of * rows_here
    slot_ids = jnp.sum(jnp.where(at_slot, local_row[:, None] + 1, 0), axis=0) - 1
    slot_map = jnp.sum(jnp.where(at_slot, plane_rank[:, None] + 1, 0), axis=0) - 1
    return (plane_of, plane_rank, slot_ids, slot_map)


def teams(near_size, far_size):
    near = [[row * near_size + place for place in range(near_size)] for row in range(far_size)]
    far = [[row * near_size + place for row in range(far_size)] for place in range(near_size)]
    return (near, far)


def sum_relations(rel_rows, near_ids, rel_count, near, far):
    near_size, far_size = len(far), len(near)
    row_count, columns = rel_rows.shape
    tiles = rel_rows.reshape(row_count, near_size, columns // near_size).transpose(1, 0, 2)
    tiles = lax.all_to_all(
        tiles, "ent", split_axis=0, concat_axis=0, axis_index_groups=near, tiled=True
    )
    hits = (near_ids[:, None] == jnp.arange(rel_count, dtype=jnp.int32)[None, :]).astype(
        jnp.bfloat16
    )
    part = contract_first(hits, tiles.reshape(near_size * row_count, columns // near_size)).astype(
        jnp.bfloat16
    )
    share = lax.psum_scatter(
        part, "ent", scatter_dimension=0, axis_index_groups=far, tiled=True
    )
    whole = lax.all_gather(share, "ent", axis=0)
    whole = whole.reshape(far_size, near_size, rel_count // far_size, columns // near_size)
    return whole.transpose(0, 2, 1, 3).reshape(rel_count, columns)


def adagrad(table, state, grad, squares):
    new_state = state + squares / (2 * RANK)
    scale = LEARN_RATE / jnp.sqrt(new_state)
    return table - grad * scale[:, None]


def per_device(entities, ent_state, buckets, relations, rel_state, triples, negatives):
    owners = lax.axis_size("ent")
    rows_here, columns_here = entities.shape
    rel_count = relations.shape[0]
    groups_here, width_neg = negatives.shape
    group_len = triples.shape[1] // groups_here
    request_count = 2 * group_len + width_neg
    slots = 8 * ((request_count + 3 * owners - 1) // (3 * owners))
    near_size = 4 if owners % 4 == 0 else 1
    far_size = owners // near_size
    most = min(near_size * slots, request_count)
    few = min(most, 16 * ((19 * slots + 127) // 128))
    ent_low = entities.astype(jnp.bfloat16)
    head_ids = triples[0].reshape(groups_here, group_len)
    tail_ids = triples[2].reshape(groups_here, group_len)
    wanted = jnp.concatenate([head_ids, tail_ids, negatives], axis=1)
    placed = [
        placement_of(wanted[index], rows_here, (near_size, far_size, slots))
        for index in range(groups_here)
    ]
    plane_of = jnp.stack([each[0] for each in placed])
    plane_rank = jnp.stack([each[1] for each in placed])
    slot_ids = jnp.stack([each[2] for each in placed])
    slot_ids = slot_ids.reshape(groups_here, far_size, near_size, slots).transpose(1, 2, 0, 3)
    slot_ids = jnp.pad(
        slot_ids, ((0, 0), (0, 0), (0, 8 - groups_here), (0, 128 - slots)), constant_values=-1
    )
    is_last_row = jnp.arange(8, dtype=jnp.int32)[:, None] == 7
    slot_ids = jnp.where(is_last_row, jnp.max(plane_rank) + 1, slot_ids)
    slot_maps = jnp.stack([each[3] for each in placed])
    slot_maps = slot_maps.reshape(groups_here, far_size, near_size * slots).transpose(1, 0, 2)
    slot_maps = jnp.pad(slot_maps, ((0, 0), (0, 8 - groups_here), (0, 0)), constant_values=-1)
    rel_rows = jnp.take(relations, triples[1], axis=0, mode="clip").astype(jnp.bfloat16)
    rel_ids = jnp.broadcast_to(triples[1][None, :], (8, triples.shape[1]))

    own_ids, line_maps, plane_rel = share_ids(slot_ids, slot_maps, rel_ids, (near_size, far_size))
    longest = jnp.max(own_ids[:, 0, 7, 0])
    place = jnp.pad(
        jnp.concatenate([plane_of, plane_rank]), ((0, 8 - 2 * groups_here), (0, 0)), constant_values=-1
    )

    def run(merged, collective_id):
        sizes = (near_size, far_size, groups_here, slots, merged, group_len, width_neg, rel_count)
        return lambda *inputs: exchange_step(inputs, sizes, collective_id)

    operands = (ent_low, own_ids, line_maps, place, rel_rows, plane_rel)
    totals, counts, rel_grad = lax.cond(longest <= few, run(few, 0), run(most, 1), *operands)
    if rel_grad.shape[0] != rel_count:
        near, far = teams(near_size, far_size)
        near_ids = lax.all_gather(triples[1], "ent", axis_index_groups=near, tiled=True)
        rel_grad = sum_relations(rel_grad, near_ids, rel_count, near, far)
    rel_grad = rel_grad.astype(jnp.float32)
    weight = REG_WEIGHT * (buckets.astype(jnp.float32) + 1.0) * counts[:, 0]
    totals = totals + weight[:, None] * 3.0 * entities * jnp.abs(entities)
    ent_squares = jnp.sum(totals * totals, axis=-1)
    ent_all, rel_all = lax.psum((ent_squares, jnp.sum(rel_grad * rel_grad, axis=-1)), "dim")
    new_relations = adagrad(relations, rel_state, rel_grad, rel_all)
    new_entities = adagrad(entities, ent_state, totals, ent_all)
    return (new_entities, new_relations)


def solution(mesh):
    placed = (
        P("ent", "dim"),
        P("ent"),
        P("ent"),
        P(None, "dim"),
        P(),
        P(None, "ent"),
        P("ent", None),
    )
    return jax.shard_map(
        per_device,
        mesh=mesh,
        in_specs=placed,
        out_specs=(P("ent", "dim"), P(None, "dim")),
        check_vma=False,
    )
```

```python
import functools

import jax
import jax.numpy as jnp
from jax import lax
from jax.experimental import pallas as pl
from jax.experimental.pallas import tpu as pltpu
from jax.sharding import PartitionSpec as P

RANK = 512
BLK = 64


LEARN_RATE = 0.1
REG_WEIGHT = 0.01
MESH = pl.DeviceIdType.MESH
VMEM_LIMIT = 60 * 1024 * 1024


def contract_first(former, latter):
    return lax.dot_general(
        former, latter, (((0,), (0,)), ((), ())), preferred_element_type=jnp.float32
    )


def contract_last(former, latter):
    return lax.dot_general(
        former, latter, (((1,), (1,)), ((), ())), preferred_element_type=jnp.float32
    )


def position(near_size):
    me = lax.axis_index("ent")
    return lax.div(me, near_size), lax.rem(me, near_size)


def greet(near_size, far_size, with_parts=True):
    far, near = position(near_size)
    parts = lax.axis_size("dim") if with_parts else 1
    barrier = pltpu.get_barrier_semaphore()
    for step in range(1, parts):
        peer = lax.rem(lax.axis_index("dim") + step, parts)
        pl.semaphore_signal(barrier, inc=1, device_id={"dim": peer}, device_id_type=MESH)
    for step in range(1, near_size):
        peer = far * near_size + lax.rem(near + step, near_size)
        pl.semaphore_signal(barrier, inc=1, device_id={"ent": peer}, device_id_type=MESH)
    for step in range(1, far_size):
        peer = lax.rem(far + step, far_size) * near_size + near
        pl.semaphore_signal(barrier, inc=1, device_id={"ent": peer}, device_id_type=MESH)
    pl.semaphore_wait(barrier, near_size + far_size + parts - 3)


def send(source, target, send_sem, recv_sem, peer, axis="ent"):
    return pltpu.make_async_remote_copy(
        src_ref=source,
        dst_ref=target,
        send_sem=send_sem,
        recv_sem=recv_sem,
        device_id={axis: peer},
        device_id_type=MESH,
    )


def line_step(index, far_size):
    return jnp.where(
        index == far_size - 1, 0, 1 + lax.rem(far_size // 2 - 1 + index, far_size - 1)
    )


def one_hot(condition):
    return condition.astype(jnp.float32).astype(jnp.bfloat16)


def dot(former, latter):
    return jnp.dot(former, latter, preferred_element_type=jnp.float32)


def swapped(values):
    return pltpu.roll(values, BLK, 1)


def spread_parts(values):
    other = swapped(values)
    first = lax.broadcasted_iota(jnp.int32, values.shape, 1) < BLK
    return jnp.where(first, values, other), jnp.where(first, -other, values)


def times(former, parts):
    return former * parts[0] + swapped(former) * parts[1]


def times_conj(former, parts):
    return former * parts[0] - swapped(former) * parts[1]


def ids_kernel(sizes, ids, maps, rel_ids, own_ids, line_maps, plane_rel, line_ids, *sems):
    near_size, far_size = sizes
    ids_ss, ids_rs, maps_ss, maps_rs, fwd_ss, fwd_rs, rid_ss, rid_rs = sems
    far, near = position(near_size)
    greet(near_size, far_size, False)

    def line_peer(step):
        there = lax.rem(far + step, far_size)
        return there, there * near_size + near

    def near_peer(step):
        there = lax.rem(near + step, near_size)
        return there, far * near_size + there

    def ids_copy(step):
        there, peer = line_peer(step)
        return send(ids.at[there], line_ids.at[far], ids_ss.at[step], ids_rs.at[step], peer)

    def maps_copy(step):
        there, peer = line_peer(step)
        return send(maps.at[there], line_maps.at[far], maps_ss.at[step], maps_rs.at[step], peer)

    def fwd_copy(step):
        there, peer = near_peer(step)
        return send(line_ids.at[:, there], own_ids.at[near], fwd_ss.at[step], fwd_rs.at[step], peer)

    def rel_ids_copy(step):
        there, peer = near_peer(step)
        return send(rel_ids, plane_rel.at[near], rid_ss.at[step], rid_rs.at[step], peer)

    for step in range(1, far_size):
        ids_copy(step).start()
    for step in range(1, far_size):
        maps_copy(step).start()
    for step in range(1, near_size):
        rel_ids_copy(step).start()
    plane_rel[near] = rel_ids[...]
    line_ids[far] = ids[far]
    line_maps[far] = maps[far]
    for step in range(1, far_size):
        ids_copy(step).wait()
    longest = line_ids[0, 0, 7:8]
    for there in range(1, far_size):
        longest = jnp.maximum(longest, line_ids[there, 0, 7:8])
    for there in range(far_size):
        for beside in range(near_size):
            line_ids[there, beside, 7:8] = longest
    for step in range(1, near_size):
        fwd_copy(step).start()
    own_ids[near] = line_ids[:, near]
    for step in range(1, near_size):
        fwd_copy(step).wait()
    for step in range(1, far_size):
        maps_copy(step).wait()
    for step in range(1, near_size):
        rel_ids_copy(step).wait()


def share_ids(ids, maps, rel_ids, sizes):
    near_size, far_size = sizes
    dma = pltpu.SemaphoreType.DMA
    vmem = pl.BlockSpec(memory_space=pltpu.VMEM)
    return pl.pallas_call(
        functools.partial(ids_kernel, sizes),
        name="share_ids",
        out_shape=(
            jax.ShapeDtypeStruct((near_size, far_size) + ids.shape[2:], jnp.int32),
            jax.ShapeDtypeStruct(maps.shape, jnp.int32),
            jax.ShapeDtypeStruct((near_size,) + rel_ids.shape, jnp.int32),
        ),
        in_specs=[vmem] * 3,
        out_specs=(vmem,) * 3,
        scratch_shapes=[pltpu.VMEM(ids.shape, jnp.int32)]
        + [dma((far_size,))] * 4
        + [dma((near_size,))] * 4,
        compiler_params=pltpu.CompilerParams(collective_id=2, has_side_effects=True),
    )(ids, maps, rel_ids)


def step_kernel(sizes, refs_in, refs_out, scratch):
    near_size, far_size, groups, slots, merged, group_len, width_neg, rel_count = sizes
    entities, own_ids, line_maps, place, rel_rows, plane_rel, weights = refs_in
    totals, ent_squares, rel_out, rel_squares = refs_out
    s = scratch
    table = s["table"]
    rows_here, columns = entities.shape
    table[...] = entities[...].astype(jnp.bfloat16)
    in_kernel_sum = "tiles_in" in s
    far, near = position(near_size)
    parts = lax.axis_size("dim")
    part_here = lax.axis_index("dim")
    greet(near_size, far_size)

    def line_peer(step):
        there = lax.rem(far + step, far_size)
        return there, there * near_size + near

    def near_peer(step):
        there = lax.rem(near + step, near_size)
        return there, far * near_size + there

    def near_copy(group, step, there):
        beside, peer = near_peer(step)
        return send(
            s["near_out"].at[group, step, there], s["near_in"].at[group, there, near],
            s["near_ss"].at[group, step, there], s["near_rs"].at[group, step, there], peer,
        )

    def look_up(group, index):
        step = lax.rem(index + 1, near_size)
        there = lax.rem(far + line_step(lax.div(index, near_size), far_size), far_size)
        beside = lax.rem(near + step, near_size)
        wanted = jnp.transpose(own_ids[beside, there])[:slots, group : group + 1]
        hits = wanted == lax.broadcasted_iota(jnp.int32, (slots, rows_here), 1)
        found = dot(one_hot(hits), table[...]).astype(jnp.bfloat16)

        @pl.when(step == 0)
        def _():
            s["near_in"][group, there, near] = found

        @pl.when(step != 0)
        def _():
            s["near_out"][group, step, there] = found
            near_copy(group, step, there).start()

    def far_copy(group, there, source):
        return send(
            s["far_out"].at[group, there], s["arrived"].at[group, source],
            s["far_ss"].at[group, there], s["far_rs"].at[group, source], there * near_size + near,
        )

    def merge(group, index):
        there = lax.rem(far + line_step(index, far_size), far_size)
        for step in range(1, near_size):
            near_copy(group, step, there).wait_recv()
        targets = line_maps[there][group : group + 1]
        picks = lax.broadcasted_iota(jnp.int32, (merged, near_size * slots), 0) == targets
        rows = s["near_in"][group, there].reshape(near_size * slots, columns)
        block = dot(one_hot(picks), rows).astype(jnp.bfloat16)

        @pl.when(there == far)
        def _():
            s["arrived"][group, far] = block

        @pl.when(there != far)
        def _():
            s["far_out"][group, there] = block
            far_copy(group, there, far).start()

    def part_copy(group, step):
        peer = lax.rem(part_here + step, parts)
        return send(
            s["part_all"].at[group, part_here], s["part_all"].at[group, part_here],
            s["part_ss"].at[group, step], s["part_rs"].at[group, step], peer, axis="dim",
        )

    def tiles_copy(group, step):
        there, peer = near_peer(step)
        span = pl.ds(group * group_len, group_len)
        return send(
            s["tiles_out"].at[there, span], s["tiles_in"].at[near, span],
            s["tiles_ss"].at[group, step], s["tiles_rs"].at[group, step], peer,
        )

    def give_copy(group, there, source):
        return send(
            s["give_out"].at[group, there], s["give_in"].at[group, source],
            s["give_ss"].at[group, there], s["give_rs"].at[group, source], there * near_size + near,
        )

    lanes = 2 * BLK
    blocks = columns // lanes

    def compute(group):
        for step in range(1, far_size):
            far_copy(group, 0, lax.rem(far + step, far_size)).wait_recv()
        place_col = jnp.transpose(place[:8])
        place_col = place_col[:, :groups] * merged + place_col[:, groups : 2 * groups]
        incoming = s["arrived"][group].reshape(far_size * merged, columns)
        request_count = 2 * group_len + width_neg
        rows = s["rows"]
        third = 256 if request_count % 256 == 0 else request_count
        for start in range(0, request_count, third):
            at = place_col[start : start + third, group : group + 1]
            picks = lax.broadcasted_iota(jnp.int32, (third, far_size * merged), 1) == at
            rows[start : start + third] = dot(one_hot(picks), incoming).astype(jnp.bfloat16)
        pos = jnp.zeros((group_len, 1), jnp.float32)
        for block in range(blocks):
            cut = slice(block * lanes, (block + 1) * lanes)
            head = rows[:group_len, cut].astype(jnp.float32)
            tail = rows[group_len : 2 * group_len, cut].astype(jnp.float32)
            rel = spread_parts(rel_rows[group * group_len : (group + 1) * group_len, cut].astype(jnp.float32))
            query = times(head, rel).astype(jnp.bfloat16)
            s["query"][:, cut] = query
            s["probe"][:, cut] = times_conj(tail, rel).astype(jnp.bfloat16)
            pos += jnp.sum(query.astype(jnp.float32) * tail, axis=1, keepdims=True)
        noise = rows[2 * group_len :]
        part = s["part_all"]
        part[group, part_here, :, :width_neg] = contract_last(s["query"][...], noise).astype(jnp.bfloat16)
        part[group, part_here, :, width_neg : 2 * width_neg] = contract_last(
            s["probe"][...], noise
        ).astype(jnp.bfloat16)
        part[group, part_here, :, 2 * width_neg :] = jnp.broadcast_to(pos, (group_len, 128)).astype(
            jnp.bfloat16
        )
        for step in range(1, parts):
            part_copy(group, step).start()
        for step in range(1, parts):
            part_copy(group, step).wait_recv()
        scores = part[group, 0].astype(jnp.float32)
        for other in range(1, parts):
            scores += part[group, other].astype(jnp.float32)
        tail_coef = jax.nn.sigmoid(scores[:, :width_neg]) * (1.0 / width_neg)
        head_coef = jax.nn.sigmoid(scores[:, width_neg : 2 * width_neg]) * (1.0 / width_neg)
        pos_coef = -jax.nn.sigmoid(-scores[:, 2 * width_neg :])
        pos_coef = pos_coef.astype(jnp.bfloat16).astype(jnp.float32)[:, :1]
        grads = s["grads"]
        grads[2 * group_len :] = (
            dot(jnp.transpose(tail_coef).astype(jnp.bfloat16), s["query"][...])
            + dot(jnp.transpose(head_coef).astype(jnp.bfloat16), s["probe"][...])
        ).astype(jnp.bfloat16)
        tail_coef = tail_coef.astype(jnp.bfloat16)
        head_coef = head_coef.astype(jnp.bfloat16)
        for block in range(blocks):
            cut = slice(block * lanes, (block + 1) * lanes)
            head = rows[:group_len, cut].astype(jnp.float32)
            tail = rows[group_len : 2 * group_len, cut].astype(jnp.float32)
            rel = spread_parts(rel_rows[group * group_len : (group + 1) * group_len, cut].astype(jnp.float32))
            noise = rows[2 * group_len :, cut]
            tail_pull = pos_coef * tail + dot(tail_coef, noise)
            head_pull = dot(head_coef, noise)
            head_side = pos_coef * head + head_pull
            grads[:group_len, cut] = times_conj(tail_pull, rel).astype(jnp.bfloat16)
            grads[group_len : 2 * group_len, cut] = times(head_side, rel).astype(jnp.bfloat16)
            rel_grad = times_conj(tail_pull, spread_parts(head)) + times_conj(tail, spread_parts(head_pull))
            span = slice(group * group_len, (group + 1) * group_len)
            if in_kernel_sum:
                per_tile = columns // near_size // lanes
                within = slice((block % per_tile) * lanes, (block % per_tile + 1) * lanes)
                s["tiles_out"][block // per_tile, span, within] = rel_grad.astype(jnp.bfloat16)
            else:
                rel_out[span, cut] = rel_grad.astype(jnp.bfloat16)

        if in_kernel_sum:
            s["tiles_in"][near, group * group_len : (group + 1) * group_len] = s["tiles_out"][
                near, group * group_len : (group + 1) * group_len
            ]
            for step in range(1, near_size):
                tiles_copy(group, step).start()

    def give_blocks(group):
        @pl.loop(0, far_size)
        def _(index):
            there = lax.rem(far + line_step(index, far_size), far_size)
            at = place[groups + group : groups + group + 1] + (place[group : group + 1] - there) * merged
            picks = lax.broadcasted_iota(jnp.int32, (merged, s["grads"].shape[0]), 0) == at
            block = dot(one_hot(picks), s["grads"][...]).astype(jnp.bfloat16)

            @pl.when(there == far)
            def _():
                s["give_in"][group, far] = block

            @pl.when(there != far)
            def _():
                s["give_out"][group, there] = block

    def give_start(group, index):
        there = lax.rem(far + line_step(index, far_size), far_size)
        give_copy(group, there, far).start()

    def hand_copy(group, step, there):
        beside, peer = near_peer(step)
        return send(
            s["hand_out"].at[group, there, beside], s["hand_in"].at[group, near, there],
            s["hand_ss"].at[group, step, there], s["hand_rs"].at[group, step, there], peer,
        )

    def spread(group, index):
        offset = jnp.where(index == 0, 0, far_size - line_step(index - 1, far_size))
        there = lax.rem(far + offset, far_size)

        @pl.when(index != 0)
        def _():
            give_copy(group, 0, there).wait_recv()

        targets = jnp.transpose(line_maps[there])[:, group : group + 1]
        picks = lax.broadcasted_iota(jnp.int32, (near_size * slots, merged), 1) == targets
        rows = dot(one_hot(picks), s["give_in"][group, there]).astype(jnp.bfloat16)
        s["hand_out"][group, there] = rows.reshape(near_size, slots, columns)
        for step in range(1, near_size):
            hand_copy(group, step, there).start()
        s["hand_in"][group, near, there] = s["hand_out"][group, there, near]

    def add_up(group, step):
        beside = lax.rem(near + near_size - step, near_size)

        @pl.when(step != 0)
        def _():
            @pl.loop(0, far_size)
            def _(there):
                hand_copy(group, step, there).wait_recv()

        if slots % 128 == 0:
            targets = jnp.concatenate(
                [own_ids[beside, there][group : group + 1, :slots] for there in range(far_size)], axis=1
            )
            rows = s["hand_in"][group, beside].reshape(far_size * slots, columns)
            chunk = 512 if rows_here % 512 == 0 else rows_here

            @pl.loop(0, rows_here // chunk)
            def _(index):
                first = pl.multiple_of(index * chunk, chunk)
                hits = lax.broadcasted_iota(jnp.int32, (chunk, far_size * slots), 0) == targets - first
                totals[pl.ds(first, chunk)] += dot(one_hot(hits), rows)

        else:

            @pl.loop(0, far_size)
            def _(there):
                targets = own_ids[beside, there][group : group + 1, :slots]
                hits = lax.broadcasted_iota(jnp.int32, (rows_here, slots), 0) == targets
                totals[...] += dot(one_hot(hits), s["hand_in"][group, beside, there])

    def add_up_all(group):
        @pl.loop(0, near_size)
        def _(step):
            add_up(group, step)

    share_len = rel_count // far_size
    beside_far = far + 1 - 2 * lax.rem(far, 2)
    across_far = lax.rem(far + 2, 4)
    diagonal_far = lax.rem(beside_far + 2, 4)
    line = lambda there: there * near_size + near
    near_x = near + 1 - 2 * lax.rem(near, 2)
    near_y = lax.rem(near + 2, 4)
    near_xy = lax.rem(near_x + 2, 4)
    plane = lambda there: far * near_size + there

    def share_rows(row):
        return pl.ds(pl.multiple_of(row * share_len, share_len), share_len)

    def halve_copy(index):
        row = beside_far if index == 0 else diagonal_far
        return send(
            s["rel_part"].at[share_rows(row)], s["share_in"].at[index],
            s["halve_ss"].at[index], s["halve_rs"].at[index], line(beside_far),
        )

    def across_copy():
        return send(
            s["share_out"], s["share_in"].at[2], s["double_ss"].at[2], s["double_rs"].at[2], line(across_far)
        )

    def rel_block(row, column, half=None):
        width = columns // near_size
        start = row * share_len
        length = share_len
        if half is not None:
            length = share_len // 2
            start = start + half * length
        return rel_out.at[
            pl.ds(pl.multiple_of(start, length), length),
            pl.ds(pl.multiple_of(column * width, width), width),
        ]

    known_rows = (far, across_far, beside_far, diagonal_far)

    def double_copy(index, row):
        peer = across_far if index == 0 else beside_far
        block = rel_block(row, near)
        return send(block, block, s["double_ss"].at[index], s["double_rs"].at[index], line(peer))

    def pass_copy(row):
        block = rel_block(row, near)
        return send(block, block, s["pass_ss"].at[0], s["pass_rs"].at[0], line(beside_far))

    def plane_copy(way, row, column):
        peer = near_x if way == 0 else near_y
        block = rel_block(row, column)
        return send(block, block, s["pg_ss"].at[way, row], s["pg_rs"].at[way, row], plane(peer))

    def relay_copy(way, row, column):
        peer = near_y if way == 0 else near_x
        block = rel_block(row, column, way)
        return send(block, block, s["relay_ss"].at[way, row], s["relay_rs"].at[way, row], plane(peer))

    def relation_parts():
        for group in range(groups):
            for step in range(1, near_size):
                tiles_copy(group, step).wait_recv()
        chunk = 512 if rel_count % 512 == 0 else rel_count

        @pl.loop(0, rel_count // chunk)
        def _(index):
            first = index * chunk
            total = jnp.zeros((chunk, columns // near_size), jnp.float32)
            for beside in range(near_size):
                at = plane_rel[beside][:1] - first
                hits = lax.broadcasted_iota(jnp.int32, (chunk, groups * group_len), 0) == at
                total += dot(one_hot(hits), s["tiles_in"][beside])
            s["rel_part"][pl.ds(pl.multiple_of(first, chunk), chunk)] = total.astype(jnp.bfloat16)

        for index in range(2):
            halve_copy(index).start()

    def part_rows(row):
        return s["rel_part"][share_rows(row)].astype(jnp.float32)

    def relation_across():
        halve_copy(1).wait_recv()
        s["share_out"][...] = (part_rows(across_far) + s["share_in"][1].astype(jnp.float32)).astype(jnp.bfloat16)
        across_copy().start()

    def relation_share():
        halve_copy(0).wait_recv()
        total = part_rows(far) + s["share_in"][0].astype(jnp.float32)
        across_copy().wait_recv()
        total += s["share_in"][2].astype(jnp.float32)
        rel_block(far, near)[...] = total.astype(jnp.bfloat16)
        double_copy(0, far).start()
        double_copy(1, far).start()
        for way in range(2):
            plane_copy(way, far, near).start()

    def relation_known(row):
        for way in range(2):
            plane_copy(way, row, near).start()

    def relation_relay(row):
        plane_copy(0, row, near_x).wait_recv()
        relay_copy(0, row, near_x).start()
        plane_copy(1, row, near_y).wait_recv()
        relay_copy(1, row, near_y).start()

    def relation_end():
        for row in known_rows:
            for way in range(2):
                relay_copy(way, row, near_xy).wait_recv()

    span = 256 if rows_here % 256 == 0 else rows_here

    def start_totals(index):
        first = pl.multiple_of(index * span, span)
        rows_of = first + lax.broadcasted_iota(jnp.int32, (span, slots), 0)
        count = jnp.zeros((span, slots), jnp.float32)
        for beside in range(near_size):
            for there in range(far_size):
                for group in range(groups):
                    targets = own_ids[beside, there][group : group + 1, :slots]
                    count += (rows_of == targets).astype(jnp.float32)
        count = jnp.sum(count, axis=1, keepdims=True)
        weight = jnp.transpose(weights[:, pl.ds(first, span)])[:, :1] * count
        own = entities[pl.ds(first, span)]
        totals[pl.ds(first, span)] = weight * own * jnp.abs(own)

    def norm_copy(which, step):
        peer = lax.rem(part_here + step, parts)
        held = s["rel_all" if which else "ent_all"].at[part_here]
        return send(held, held, s["norm_ss"].at[which, step], s["norm_rs"].at[which, step], peer, axis="dim")

    def norm_start(which):
        values = rel_out if which else totals
        held = s["rel_all" if which else "ent_all"]

        @pl.loop(0, values.shape[0] // span)
        def _(index):
            first = pl.multiple_of(index * span, span)
            block = values[pl.ds(first, span)].astype(jnp.float32)
            square = jnp.sum(block * block, axis=1, keepdims=True)
            held[part_here, :, pl.ds(first, span)] = jnp.transpose(jnp.broadcast_to(square, (span, 8)))

        for step in range(1, parts):
            norm_copy(which, step).start()

    def norm_end(which):
        held = s["rel_all" if which else "ent_all"]
        for step in range(1, parts):
            norm_copy(which, step).wait()
        total = held[0]
        for other in range(1, parts):
            total += held[other]
        (rel_squares if which else ent_squares)[...] = total

    @pl.loop(0, far_size * near_size)
    def _(index):
        look_up(0, index)

    for group in range(1, groups):

        @pl.loop(0, far_size)
        def _(index):
            @pl.loop(0, near_size)
            def _(part):
                look_up(group, index * near_size + part)

            merge(group - 1, index)

    @pl.loop(0, rows_here // span)
    def _(index):
        start_totals(index)

    last = groups - 1
    early = far_size // 2 if groups > 1 else far_size

    @pl.loop(0, early)
    def _(index):
        merge(last, index)

    for group in range(last):
        compute(group)
        if group == 0:

            @pl.loop(early, far_size)
            def _(index):
                merge(last, index)

        give_blocks(group)
        for index in range(far_size - 1):
            give_start(group, index)

    if last > 0:
        spread(0, 0)
    compute(last)
    if in_kernel_sum:
        for index in range(1, far_size - 1):
            if last > 0:
                spread(0, index)
        relation_parts()
        give_blocks(last)
        give_start(last, 0)
        if last > 0:
            spread(0, far_size - 1)
        relation_across()
        spread(last, 0)
        relation_share()
        give_start(last, 1)
        give_start(last, 2)
        if last > 0:
            add_up_all(0)
        double_copy(0, across_far).wait_recv()
        pass_copy(across_far).start()
        relation_known(across_far)
        spread(last, 1)
        double_copy(1, beside_far).wait_recv()
        relation_known(beside_far)
        relation_relay(far)
        pass_copy(diagonal_far).wait_recv()
        relation_known(diagonal_far)
        relation_relay(across_far)
        spread(last, 2)
        relation_relay(beside_far)
        spread(last, 3)
        relation_relay(diagonal_far)
        relation_end()
        norm_start(1)
        add_up_all(last)
        norm_start(0)
        norm_end(1)
    else:
        give_blocks(last)
        for index in range(far_size - 1):
            give_start(last, index)
        for group in range(groups):

            @pl.loop(1 if group == 0 and last > 0 else 0, far_size)
            def _(index):
                spread(group, index)

        for group in range(groups):
            add_up_all(group)
        norm_start(0)
        rel_squares[...] = jnp.zeros_like(rel_squares)
    norm_end(0)

    for group in range(groups):
        for step in range(1, far_size):
            there = lax.rem(far + step, far_size)
            far_copy(group, there, 0).wait_send()
            give_copy(group, there, 0).wait_send()
        for step in range(1, parts):
            part_copy(group, step).wait_send()
        for step in range(1, near_size):

            @pl.loop(0, far_size)
            def _(there):
                near_copy(group, step, there).wait_send()
                hand_copy(group, step, there).wait_send()

    if in_kernel_sum:
        for step in range(1, near_size):
            for group in range(groups):
                tiles_copy(group, step).wait_send()
        for index in range(2):
            halve_copy(index).wait_send()
            double_copy(index, far).wait_send()
        across_copy().wait_send()
        pass_copy(across_far).wait_send()
        for row in known_rows:
            for way in range(2):
                plane_copy(way, row, near).wait_send()
                relay_copy(way, row, near).wait_send()


def sums_in_kernel(columns, near_size, far_size):
    return near_size == 4 and far_size == 4 and columns % (2 * BLK * near_size) == 0


def exchange_step(inputs, sizes, collective_id):
    near_size, far_size, groups, slots, merged, group_len, width_neg, rel_count = sizes
    rows_here, columns = inputs[0].shape
    parts = lax.axis_size("dim")
    dma = pltpu.SemaphoreType.DMA
    low = jnp.bfloat16
    vmem = pl.BlockSpec(memory_space=pltpu.VMEM)
    request_count = 2 * group_len + width_neg
    in_kernel_sum = sums_in_kernel(columns, near_size, far_size)
    scratch = {
        "table": pltpu.VMEM((rows_here, columns), low),
        "ent_all": pltpu.VMEM((parts, 8, rows_here), jnp.float32),
        "near_out": pltpu.VMEM((groups, near_size, far_size, slots, columns), low),
        "near_in": pltpu.VMEM((groups, far_size, near_size, slots, columns), low),
        "far_out": pltpu.VMEM((groups, far_size, merged, columns), low),
        "arrived": pltpu.VMEM((groups, far_size, merged, columns), low),
        "rows": pltpu.VMEM((request_count, columns), low),
        "grads": pltpu.VMEM((request_count, columns), low),
        "query": pltpu.VMEM((group_len, columns), low),
        "probe": pltpu.VMEM((group_len, columns), low),
        "part_all": pltpu.VMEM((groups, parts, group_len, 2 * width_neg + 128), low),
        "give_out": pltpu.VMEM((groups, far_size, merged, columns), low),
        "give_in": pltpu.VMEM((groups, far_size, merged, columns), low),
        "hand_out": pltpu.VMEM((groups, far_size, near_size, slots, columns), low),
        "hand_in": pltpu.VMEM((groups, near_size, far_size, slots, columns), low),
    }
    for name, shape in (
        ("near", (groups, near_size, far_size)), ("far", (groups, far_size)),
        ("part", (groups, parts)), ("give", (groups, far_size)), ("norm", (2, parts)),
        ("hand", (groups, near_size, far_size)),
    ):
        scratch[name + "_ss"] = dma(shape)
        scratch[name + "_rs"] = dma(shape)
    if in_kernel_sum:
        width = columns // near_size
        scratch["rel_all"] = pltpu.VMEM((parts, 8, rel_count), jnp.float32)
        scratch["tiles_out"] = pltpu.VMEM((near_size, groups * group_len, width), low)
        scratch["tiles_in"] = pltpu.VMEM((near_size, groups * group_len, width), low)
        scratch["rel_part"] = pltpu.VMEM((rel_count, width), low)
        scratch["share_in"] = pltpu.VMEM((3, rel_count // far_size, width), low)
        scratch["share_out"] = pltpu.VMEM((rel_count // far_size, width), low)
        for name, shape in (
            ("tiles", (groups, near_size)), ("halve", (2,)), ("double", (3,)), ("pass", (1,)),
            ("pg", (2, far_size)), ("relay", (2, far_size)),
        ):
            scratch[name + "_ss"] = dma(shape)
            scratch[name + "_rs"] = dma(shape)
    names = tuple(scratch)
    rel_rows_out = rel_count if in_kernel_sum else groups * group_len

    def kernel(*refs):
        step_kernel(sizes, refs[:7], refs[7:11], dict(zip(names, refs[11:])))

    return pl.pallas_call(
        kernel,
        name="exchange_step",
        out_shape=(
            jax.ShapeDtypeStruct((rows_here, columns), jnp.float32),
            jax.ShapeDtypeStruct((8, rows_here), jnp.float32),
            jax.ShapeDtypeStruct((rel_rows_out, columns), low),
            jax.ShapeDtypeStruct((8, rel_count), jnp.float32),
        ),
        in_specs=[vmem] * 7,
        out_specs=(vmem,) * 4,
        scratch_shapes=list(scratch.values()),
        compiler_params=pltpu.CompilerParams(
            collective_id=collective_id, has_side_effects=True, vmem_limit_bytes=VMEM_LIMIT
        ),
    )(*inputs)


def placement_of(wanted_row, rows_here, sizes):
    near_size, far_size, slots = sizes
    owners = near_size * far_size
    request_count = wanted_row.shape[0]
    owner_of = wanted_row // rows_here
    owner_hits = (owner_of[:, None] == jnp.arange(owners, dtype=jnp.int32)[None, :]).astype(
        jnp.bfloat16
    )
    order = jnp.arange(request_count, dtype=jnp.int32)
    earlier = (order[:, None] > order[None, :]).astype(jnp.bfloat16)
    before = jnp.dot(earlier, owner_hits, preferred_element_type=jnp.float32)
    slot_rank = jnp.sum(before * owner_hits.astype(jnp.float32), axis=-1).astype(jnp.int32)
    plane_of = owner_of // near_size
    same_plane = (
        plane_of[:, None] == (jnp.arange(owners, dtype=jnp.int32) // near_size)[None, :]
    ).astype(jnp.float32)
    plane_rank = jnp.sum(before * same_plane, axis=-1).astype(jnp.int32)
    slot_flat = owner_of * slots + slot_rank
    at_slot = slot_flat[:, None] == jnp.arange(owners * slots, dtype=jnp.int32)[None, :]
    local_row = wanted_row - owner_of * rows_here
    slot_ids = jnp.sum(jnp.where(at_slot, local_row[:, None] + 1, 0), axis=0) - 1
    slot_map = jnp.sum(jnp.where(at_slot, plane_rank[:, None] + 1, 0), axis=0) - 1
    return (plane_of, plane_rank, slot_ids, slot_map)


def teams(near_size, far_size):
    near = [[row * near_size + place for place in range(near_size)] for row in range(far_size)]
    far = [[row * near_size + place for row in range(far_size)] for place in range(near_size)]
    return (near, far)


def sum_relations(rel_rows, near_ids, rel_count, near, far):
    near_size, far_size = len(far), len(near)
    row_count, columns = rel_rows.shape
    tiles = rel_rows.reshape(row_count, near_size, columns // near_size).transpose(1, 0, 2)
    tiles = lax.all_to_all(
        tiles, "ent", split_axis=0, concat_axis=0, axis_index_groups=near, tiled=True
    )
    hits = (near_ids[:, None] == jnp.arange(rel_count, dtype=jnp.int32)[None, :]).astype(
        jnp.bfloat16
    )
    part = contract_first(hits, tiles.reshape(near_size * row_count, columns // near_size)).astype(
        jnp.bfloat16
    )
    share = lax.psum_scatter(
        part, "ent", scatter_dimension=0, axis_index_groups=far, tiled=True
    )
    whole = lax.all_gather(share, "ent", axis=0)
    whole = whole.reshape(far_size, near_size, rel_count // far_size, columns // near_size)
    return whole.transpose(0, 2, 1, 3).reshape(rel_count, columns)


def adagrad(table, state, grad, squares):
    new_state = state + squares / (2 * RANK)
    scale = LEARN_RATE / jnp.sqrt(new_state)
    return table - grad * scale[:, None]


def per_device(entities, ent_state, buckets, relations, rel_state, triples, negatives):
    owners = lax.axis_size("ent")
    rows_here, columns_here = entities.shape
    rel_count = relations.shape[0]
    groups_here, width_neg = negatives.shape
    group_len = triples.shape[1] // groups_here
    request_count = 2 * group_len + width_neg
    slots = 8 * ((request_count + 3 * owners - 1) // (3 * owners))
    near_size = 4 if owners % 4 == 0 else 1
    far_size = owners // near_size
    most = min(near_size * slots, request_count)
    few = min(most, 16 * ((19 * slots + 127) // 128))
    head_ids = triples[0].reshape(groups_here, group_len)
    tail_ids = triples[2].reshape(groups_here, group_len)
    wanted = jnp.concatenate([head_ids, tail_ids, negatives], axis=1)
    placed = [
        placement_of(wanted[index], rows_here, (near_size, far_size, slots))
        for index in range(groups_here)
    ]
    plane_of = jnp.stack([each[0] for each in placed])
    plane_rank = jnp.stack([each[1] for each in placed])
    slot_ids = jnp.stack([each[2] for each in placed])
    slot_ids = slot_ids.reshape(groups_here, far_size, near_size, slots).transpose(1, 2, 0, 3)
    slot_ids = jnp.pad(
        slot_ids, ((0, 0), (0, 0), (0, 8 - groups_here), (0, 128 - slots)), constant_values=-1
    )
    is_last_row = jnp.arange(8, dtype=jnp.int32)[:, None] == 7
    slot_ids = jnp.where(is_last_row, jnp.max(plane_rank) + 1, slot_ids)
    slot_maps = jnp.stack([each[3] for each in placed])
    slot_maps = slot_maps.reshape(groups_here, far_size, near_size * slots).transpose(1, 0, 2)
    slot_maps = jnp.pad(slot_maps, ((0, 0), (0, 8 - groups_here), (0, 0)), constant_values=-1)
    rel_rows = jnp.take(relations, triples[1], axis=0, mode="clip").astype(jnp.bfloat16)
    rel_ids = jnp.broadcast_to(triples[1][None, :], (8, triples.shape[1]))

    own_ids, line_maps, plane_rel = share_ids(slot_ids, slot_maps, rel_ids, (near_size, far_size))
    longest = jnp.max(own_ids[:, 0, 7, 0])
    place = jnp.pad(
        jnp.concatenate([plane_of, plane_rank]), ((0, 8 - 2 * groups_here), (0, 0)), constant_values=-1
    )

    def run(merged, collective_id):
        sizes = (near_size, far_size, groups_here, slots, merged, group_len, width_neg, rel_count)
        return lambda *inputs: exchange_step(inputs, sizes, collective_id)

    weights = 3.0 * REG_WEIGHT * (buckets.astype(jnp.float32) + 1.0)
    weights = jnp.broadcast_to(weights[None, :], (8, rows_here))
    operands = (entities, own_ids, line_maps, place, rel_rows, plane_rel, weights)
    totals, ent_all, rel_grad, rel_all = lax.cond(
        longest <= few, run(few, 0), run(most, 1), *operands
    )
    if rel_grad.shape[0] != rel_count:
        near, far = teams(near_size, far_size)
        near_ids = lax.all_gather(triples[1], "ent", axis_index_groups=near, tiled=True)
        rel_grad = sum_relations(rel_grad, near_ids, rel_count, near, far)
        rel_all = lax.psum(jnp.sum(rel_grad.astype(jnp.float32) ** 2, axis=-1), "dim")[None]
    rel_grad = rel_grad.astype(jnp.float32)
    new_relations = adagrad(relations, rel_state, rel_grad, rel_all[0])
    new_entities = adagrad(entities, ent_state, totals, ent_all[0])
    return (new_entities, new_relations)


def solution(mesh):
    placed = (
        P("ent", "dim"),
        P("ent"),
        P("ent"),
        P(None, "dim"),
        P(),
        P(None, "ent"),
        P("ent", None),
    )
    return jax.shard_map(
        per_device,
        mesh=mesh,
        in_specs=placed,
        out_specs=(P("ent", "dim"), P(None, "dim")),
        check_vma=False,
    )
```

```python
import functools

import jax
import jax.numpy as jnp
from jax import lax
from jax.experimental import pallas as pl
from jax.experimental.pallas import tpu as pltpu
from jax.sharding import PartitionSpec as P

RANK = 512
BLK = 64


LEARN_RATE = 0.1
REG_WEIGHT = 0.01
MESH = pl.DeviceIdType.MESH
VMEM_LIMIT = 60 * 1024 * 1024


def contract_first(former, latter):
    return lax.dot_general(
        former, latter, (((0,), (0,)), ((), ())), preferred_element_type=jnp.float32
    )


def contract_last(former, latter):
    return lax.dot_general(
        former, latter, (((1,), (1,)), ((), ())), preferred_element_type=jnp.float32
    )


def position(near_size):
    me = lax.axis_index("ent")
    return lax.div(me, near_size), lax.rem(me, near_size)


def greet(near_size, far_size, with_parts=True):
    far, near = position(near_size)
    parts = lax.axis_size("dim") if with_parts else 1
    barrier = pltpu.get_barrier_semaphore()
    for step in range(1, parts):
        peer = lax.rem(lax.axis_index("dim") + step, parts)
        pl.semaphore_signal(barrier, inc=1, device_id={"dim": peer}, device_id_type=MESH)
    for step in range(1, near_size):
        peer = far * near_size + lax.rem(near + step, near_size)
        pl.semaphore_signal(barrier, inc=1, device_id={"ent": peer}, device_id_type=MESH)
    for step in range(1, far_size):
        peer = lax.rem(far + step, far_size) * near_size + near
        pl.semaphore_signal(barrier, inc=1, device_id={"ent": peer}, device_id_type=MESH)
    pl.semaphore_wait(barrier, near_size + far_size + parts - 3)


def send(source, target, send_sem, recv_sem, peer, axis="ent"):
    return pltpu.make_async_remote_copy(
        src_ref=source,
        dst_ref=target,
        send_sem=send_sem,
        recv_sem=recv_sem,
        device_id={axis: peer},
        device_id_type=MESH,
    )


def line_step(index, far_size):
    return jnp.where(
        index == far_size - 1, 0, 1 + lax.rem(far_size // 2 - 1 + index, far_size - 1)
    )


def one_hot(condition):
    return condition.astype(jnp.float32).astype(jnp.bfloat16)


def dot(former, latter):
    return jnp.dot(former, latter, preferred_element_type=jnp.float32)


def swapped(values):
    return pltpu.roll(values, BLK, 1)


def spread_parts(values):
    other = swapped(values)
    first = lax.broadcasted_iota(jnp.int32, values.shape, 1) < BLK
    return jnp.where(first, values, other), jnp.where(first, -other, values)


def times(former, parts):
    return former * parts[0] + swapped(former) * parts[1]


def times_conj(former, parts):
    return former * parts[0] - swapped(former) * parts[1]


def ids_kernel(sizes, ids, maps, rel_ids, own_ids, line_maps, plane_rel, line_ids, ids_out, *sems):
    near_size, far_size = sizes
    ids_ss, ids_rs, maps_ss, maps_rs, fwd_ss, fwd_rs, rid_ss, rid_rs = sems
    far, near = position(near_size)
    greet(near_size, far_size, False)

    def line_peer(step):
        there = lax.rem(far + step, far_size)
        return there, there * near_size + near

    def near_peer(step):
        there = lax.rem(near + step, near_size)
        return there, far * near_size + there

    def ids_copy(step):
        there, peer = line_peer(step)
        return send(ids_out.at[there], line_ids.at[far], ids_ss.at[step], ids_rs.at[step], peer)

    def maps_copy(step):
        there, peer = line_peer(step)
        return send(maps.at[there], line_maps.at[far], maps_ss.at[step], maps_rs.at[step], peer)

    def fwd_copy(step):
        there, peer = near_peer(step)
        return send(line_ids.at[:, there], own_ids.at[near], fwd_ss.at[step], fwd_rs.at[step], peer)

    def rel_ids_copy(step):
        there, peer = near_peer(step)
        return send(rel_ids, plane_rel.at[near], rid_ss.at[step], rid_rs.at[step], peer)

    longest = jnp.full((8, 128), -1, jnp.int32)
    for there in range(far_size):
        for first in range(0, maps.shape[2], 128):
            longest = jnp.maximum(longest, maps[there, :, first : first + 128])
    longest = jnp.max(longest + 1, axis=0, keepdims=True)
    is_last = lax.broadcasted_iota(jnp.int32, (8, 128), 0) == 7
    for there in range(far_size):
        for beside in range(near_size):
            ids_out[there, beside] = jnp.where(is_last, longest, ids[there, beside])
    for step in range(1, far_size):
        ids_copy(step).start()
    for step in range(1, far_size):
        maps_copy(step).start()
    for step in range(1, near_size):
        rel_ids_copy(step).start()
    plane_rel[near] = rel_ids[...]
    line_ids[far] = ids_out[far]
    line_maps[far] = maps[far]
    for step in range(1, far_size):
        ids_copy(step).wait()
    longest = line_ids[0, 0, 7:8]
    for there in range(1, far_size):
        longest = jnp.maximum(longest, line_ids[there, 0, 7:8])
    for there in range(far_size):
        for beside in range(near_size):
            line_ids[there, beside, 7:8] = longest
    for step in range(1, near_size):
        fwd_copy(step).start()
    own_ids[near] = line_ids[:, near]
    for step in range(1, near_size):
        fwd_copy(step).wait()
    for step in range(1, far_size):
        maps_copy(step).wait()
    for step in range(1, near_size):
        rel_ids_copy(step).wait()


def share_ids(ids, maps, rel_ids, sizes):
    near_size, far_size = sizes
    dma = pltpu.SemaphoreType.DMA
    vmem = pl.BlockSpec(memory_space=pltpu.VMEM)
    return pl.pallas_call(
        functools.partial(ids_kernel, sizes),
        name="share_ids",
        out_shape=(
            jax.ShapeDtypeStruct((near_size, far_size) + ids.shape[2:], jnp.int32),
            jax.ShapeDtypeStruct(maps.shape, jnp.int32),
            jax.ShapeDtypeStruct((near_size,) + rel_ids.shape, jnp.int32),
        ),
        in_specs=[vmem] * 3,
        out_specs=(vmem,) * 3,
        scratch_shapes=[pltpu.VMEM(ids.shape, jnp.int32)] * 2
        + [dma((far_size,))] * 4
        + [dma((near_size,))] * 4,
        compiler_params=pltpu.CompilerParams(collective_id=2, has_side_effects=True),
    )(ids, maps, rel_ids)


def step_kernel(sizes, refs_in, refs_out, scratch):
    near_size, far_size, groups, slots, merged, group_len, width_neg, rel_count = sizes
    entities, own_ids, line_maps, place, rel_rows, plane_rel, weights = refs_in
    totals, ent_squares, rel_out, rel_squares = refs_out
    s = scratch
    table = s["table"]
    rows_here, columns = entities.shape
    table[...] = entities[...].astype(jnp.bfloat16)
    in_kernel_sum = "tiles_in" in s
    far, near = position(near_size)
    parts = lax.axis_size("dim")
    part_here = lax.axis_index("dim")
    greet(near_size, far_size)

    def line_peer(step):
        there = lax.rem(far + step, far_size)
        return there, there * near_size + near

    def near_peer(step):
        there = lax.rem(near + step, near_size)
        return there, far * near_size + there

    def near_copy(group, step, there):
        beside, peer = near_peer(step)
        return send(
            s["near_out"].at[group, step, there], s["near_in"].at[group, there, near],
            s["near_ss"].at[group, step, there], s["near_rs"].at[group, step, there], peer,
        )

    def look_up(group, index):
        step = lax.rem(index + 1, near_size)
        there = lax.rem(far + line_step(lax.div(index, near_size), far_size), far_size)
        beside = lax.rem(near + step, near_size)
        wanted = jnp.transpose(own_ids[beside, there])[:slots, group : group + 1]
        hits = wanted == lax.broadcasted_iota(jnp.int32, (slots, rows_here), 1)
        found = dot(one_hot(hits), table[...]).astype(jnp.bfloat16)

        @pl.when(step == 0)
        def _():
            s["near_in"][group, there, near] = found

        @pl.when(step != 0)
        def _():
            s["near_out"][group, step, there] = found
            near_copy(group, step, there).start()

    def far_copy(group, there, source):
        return send(
            s["far_out"].at[group, there], s["arrived"].at[group, source],
            s["far_ss"].at[group, there], s["far_rs"].at[group, source], there * near_size + near,
        )

    def merge(group, index):
        there = lax.rem(far + line_step(index, far_size), far_size)
        for step in range(1, near_size):
            near_copy(group, step, there).wait_recv()
        targets = line_maps[there][group : group + 1]
        picks = lax.broadcasted_iota(jnp.int32, (merged, near_size * slots), 0) == targets
        rows = s["near_in"][group, there].reshape(near_size * slots, columns)
        block = dot(one_hot(picks), rows).astype(jnp.bfloat16)

        @pl.when(there == far)
        def _():
            s["arrived"][group, far] = block

        @pl.when(there != far)
        def _():
            s["far_out"][group, there] = block
            far_copy(group, there, far).start()

    def part_copy(group, step):
        peer = lax.rem(part_here + step, parts)
        return send(
            s["part_all"].at[group, part_here], s["part_all"].at[group, part_here],
            s["part_ss"].at[group, step], s["part_rs"].at[group, step], peer, axis="dim",
        )

    def tiles_copy(group, step):
        there, peer = near_peer(step)
        span = pl.ds(group * group_len, group_len)
        return send(
            s["tiles_out"].at[there, span], s["tiles_in"].at[near, span],
            s["tiles_ss"].at[group, step], s["tiles_rs"].at[group, step], peer,
        )

    def give_copy(group, there, source):
        return send(
            s["give_out"].at[group, there], s["give_in"].at[group, source],
            s["give_ss"].at[group, there], s["give_rs"].at[group, source], there * near_size + near,
        )

    lanes = 2 * BLK
    blocks = columns // lanes

    def compute(group):
        for step in range(1, far_size):
            far_copy(group, 0, lax.rem(far + step, far_size)).wait_recv()
        place_col = jnp.transpose(place[:8])
        place_col = place_col[:, :groups] * merged + place_col[:, groups : 2 * groups]
        incoming = s["arrived"][group].reshape(far_size * merged, columns)
        request_count = 2 * group_len + width_neg
        rows = s["rows"]
        third = 256 if request_count % 256 == 0 else request_count
        for start in range(0, request_count, third):
            at = place_col[start : start + third, group : group + 1]
            picks = lax.broadcasted_iota(jnp.int32, (third, far_size * merged), 1) == at
            rows[start : start + third] = dot(one_hot(picks), incoming).astype(jnp.bfloat16)
        pos = jnp.zeros((group_len, 1), jnp.float32)
        for block in range(blocks):
            cut = slice(block * lanes, (block + 1) * lanes)
            head = rows[:group_len, cut].astype(jnp.float32)
            tail = rows[group_len : 2 * group_len, cut].astype(jnp.float32)
            rel = spread_parts(rel_rows[group * group_len : (group + 1) * group_len, cut].astype(jnp.float32))
            query = times(head, rel).astype(jnp.bfloat16)
            s["query"][:, cut] = query
            s["probe"][:, cut] = times_conj(tail, rel).astype(jnp.bfloat16)
            pos += jnp.sum(query.astype(jnp.float32) * tail, axis=1, keepdims=True)
        noise = rows[2 * group_len :]
        part = s["part_all"]
        part[group, part_here, :, :width_neg] = contract_last(s["query"][...], noise).astype(jnp.bfloat16)
        part[group, part_here, :, width_neg : 2 * width_neg] = contract_last(
            s["probe"][...], noise
        ).astype(jnp.bfloat16)
        part[group, part_here, :, 2 * width_neg :] = jnp.broadcast_to(pos, (group_len, 128)).astype(
            jnp.bfloat16
        )
        for step in range(1, parts):
            part_copy(group, step).start()
        for step in range(1, parts):
            part_copy(group, step).wait_recv()
        scores = part[group, 0].astype(jnp.float32)
        for other in range(1, parts):
            scores += part[group, other].astype(jnp.float32)
        tail_coef = jax.nn.sigmoid(scores[:, :width_neg]) * (1.0 / width_neg)
        head_coef = jax.nn.sigmoid(scores[:, width_neg : 2 * width_neg]) * (1.0 / width_neg)
        pos_coef = -jax.nn.sigmoid(-scores[:, 2 * width_neg :])
        pos_coef = pos_coef.astype(jnp.bfloat16).astype(jnp.float32)[:, :1]
        grads = s["grads"]
        grads[2 * group_len :] = (
            dot(jnp.transpose(tail_coef).astype(jnp.bfloat16), s["query"][...])
            + dot(jnp.transpose(head_coef).astype(jnp.bfloat16), s["probe"][...])
        ).astype(jnp.bfloat16)
        tail_coef = tail_coef.astype(jnp.bfloat16)
        head_coef = head_coef.astype(jnp.bfloat16)
        for block in range(blocks):
            cut = slice(block * lanes, (block + 1) * lanes)
            head = rows[:group_len, cut].astype(jnp.float32)
            tail = rows[group_len : 2 * group_len, cut].astype(jnp.float32)
            rel = spread_parts(rel_rows[group * group_len : (group + 1) * group_len, cut].astype(jnp.float32))
            noise = rows[2 * group_len :, cut]
            tail_pull = pos_coef * tail + dot(tail_coef, noise)
            head_pull = dot(head_coef, noise)
            head_side = pos_coef * head + head_pull
            grads[:group_len, cut] = times_conj(tail_pull, rel).astype(jnp.bfloat16)
            grads[group_len : 2 * group_len, cut] = times(head_side, rel).astype(jnp.bfloat16)
            rel_grad = times_conj(tail_pull, spread_parts(head)) + times_conj(tail, spread_parts(head_pull))
            span = slice(group * group_len, (group + 1) * group_len)
            if in_kernel_sum:
                per_tile = columns // near_size // lanes
                within = slice((block % per_tile) * lanes, (block % per_tile + 1) * lanes)
                s["tiles_out"][block // per_tile, span, within] = rel_grad.astype(jnp.bfloat16)
            else:
                rel_out[span, cut] = rel_grad.astype(jnp.bfloat16)

        if in_kernel_sum:
            s["tiles_in"][near, group * group_len : (group + 1) * group_len] = s["tiles_out"][
                near, group * group_len : (group + 1) * group_len
            ]
            for step in range(1, near_size):
                tiles_copy(group, step).start()

    def give_blocks(group):
        @pl.loop(0, far_size)
        def _(index):
            there = lax.rem(far + line_step(index, far_size), far_size)
            at = place[groups + group : groups + group + 1] + (place[group : group + 1] - there) * merged
            picks = lax.broadcasted_iota(jnp.int32, (merged, s["grads"].shape[0]), 0) == at
            block = dot(one_hot(picks), s["grads"][...]).astype(jnp.bfloat16)

            @pl.when(there == far)
            def _():
                s["give_in"][group, far] = block

            @pl.when(there != far)
            def _():
                s["give_out"][group, there] = block

    def give_start(group, index):
        there = lax.rem(far + line_step(index, far_size), far_size)
        give_copy(group, there, far).start()

    def hand_copy(group, step, there):
        beside, peer = near_peer(step)
        return send(
            s["hand_out"].at[group, there, beside], s["hand_in"].at[group, there, near],
            s["hand_ss"].at[group, step, there], s["hand_rs"].at[group, step, there], peer,
        )

    def spread(group, index):
        offset = jnp.where(index == 0, 0, far_size - line_step(index - 1, far_size))
        there = lax.rem(far + offset, far_size)

        @pl.when(index != 0)
        def _():
            give_copy(group, 0, there).wait_recv()

        targets = jnp.transpose(line_maps[there])[:, group : group + 1]
        picks = lax.broadcasted_iota(jnp.int32, (near_size * slots, merged), 1) == targets
        rows = dot(one_hot(picks), s["give_in"][group, there]).astype(jnp.bfloat16)
        s["hand_out"][group, there] = rows.reshape(near_size, slots, columns)
        for step in range(1, near_size):
            hand_copy(group, step, there).start()
        s["hand_in"][group, there, near] = s["hand_out"][group, there, near]

    def add_up(group, index):
        offset = jnp.where(index == 0, 0, far_size - line_step(index - 1, far_size))
        there = lax.rem(far + offset, far_size)
        for step in range(1, near_size):
            hand_copy(group, step, there).wait_recv()
        if slots % 128 == 0:
            targets = jnp.concatenate(
                [own_ids[beside, there][group : group + 1, :slots] for beside in range(near_size)], axis=1
            )
            rows = s["hand_in"][group, there].reshape(near_size * slots, columns)
            chunk = 512 if rows_here % 512 == 0 else rows_here

            @pl.loop(0, rows_here // chunk)
            def _(part):
                first = pl.multiple_of(part * chunk, chunk)
                hits = lax.broadcasted_iota(jnp.int32, (chunk, near_size * slots), 0) == targets - first
                totals[pl.ds(first, chunk)] += dot(one_hot(hits), rows)

        else:

            @pl.loop(0, near_size)
            def _(beside):
                targets = own_ids[beside, there][group : group + 1, :slots]
                hits = lax.broadcasted_iota(jnp.int32, (rows_here, slots), 0) == targets
                totals[...] += dot(one_hot(hits), s["hand_in"][group, there, beside])

    def add_up_all(group):
        @pl.loop(0, far_size)
        def _(index):
            add_up(group, index)

    def span_of(act, group, first, end):
        @pl.loop(first, end)
        def _(index):
            act(group, index)

    share_len = rel_count // far_size
    beside_far = far + 1 - 2 * lax.rem(far, 2)
    across_far = lax.rem(far + 2, 4)
    diagonal_far = lax.rem(beside_far + 2, 4)
    line = lambda there: there * near_size + near
    near_x = near + 1 - 2 * lax.rem(near, 2)
    near_y = lax.rem(near + 2, 4)
    near_xy = lax.rem(near_x + 2, 4)
    plane = lambda there: far * near_size + there

    def share_rows(row):
        return pl.ds(pl.multiple_of(row * share_len, share_len), share_len)

    def halve_copy(index):
        row = beside_far if index == 0 else diagonal_far
        return send(
            s["rel_part"].at[share_rows(row)], s["share_in"].at[index],
            s["halve_ss"].at[index], s["halve_rs"].at[index], line(beside_far),
        )

    def across_copy():
        return send(
            s["share_out"], s["share_in"].at[2], s["double_ss"].at[2], s["double_rs"].at[2], line(across_far)
        )

    def rel_block(row, column, half=None):
        width = columns // near_size
        start = row * share_len
        length = share_len
        if half is not None:
            length = share_len // 2
            start = start + half * length
        return rel_out.at[
            pl.ds(pl.multiple_of(start, length), length),
            pl.ds(pl.multiple_of(column * width, width), width),
        ]

    known_rows = (far, across_far, beside_far, diagonal_far)

    def double_copy(index, row):
        peer = across_far if index == 0 else beside_far
        block = rel_block(row, near)
        return send(block, block, s["double_ss"].at[index], s["double_rs"].at[index], line(peer))

    def pass_copy(row):
        block = rel_block(row, near)
        return send(block, block, s["pass_ss"].at[0], s["pass_rs"].at[0], line(beside_far))

    def plane_copy(way, row, column):
        peer = near_x if way == 0 else near_y
        block = rel_block(row, column)
        return send(block, block, s["pg_ss"].at[way, row], s["pg_rs"].at[way, row], plane(peer))

    def relay_copy(way, row, column):
        peer = near_y if way == 0 else near_x
        block = rel_block(row, column, way)
        return send(block, block, s["relay_ss"].at[way, row], s["relay_rs"].at[way, row], plane(peer))

    def relation_parts(group):
        for step in range(1, near_size):
            tiles_copy(group, step).wait_recv()
        chunk = 512 if rel_count % 512 == 0 else rel_count
        of_group = slice(group * group_len, (group + 1) * group_len)

        @pl.loop(0, rel_count // chunk)
        def _(index):
            first = pl.multiple_of(index * chunk, chunk)
            total = jnp.zeros((chunk, columns // near_size), jnp.float32)
            if group > 0:
                total += s["rel_part"][pl.ds(first, chunk)].astype(jnp.float32)
            for beside in range(near_size):
                at = plane_rel[beside][:1, of_group] - first
                hits = lax.broadcasted_iota(jnp.int32, (chunk, group_len), 0) == at
                total += dot(one_hot(hits), s["tiles_in"][beside, of_group])
            s["rel_part"][pl.ds(first, chunk)] = total.astype(jnp.bfloat16)

    def relation_halve():
        for index in (1, 0):
            halve_copy(index).start()

    def part_rows(row):
        return s["rel_part"][share_rows(row)].astype(jnp.float32)

    def relation_across():
        halve_copy(1).wait_recv()
        s["share_out"][...] = (part_rows(across_far) + s["share_in"][1].astype(jnp.float32)).astype(jnp.bfloat16)
        across_copy().start()

    def relation_share():
        halve_copy(0).wait_recv()
        total = part_rows(far) + s["share_in"][0].astype(jnp.float32)
        across_copy().wait_recv()
        total += s["share_in"][2].astype(jnp.float32)
        rel_block(far, near)[...] = total.astype(jnp.bfloat16)
        double_copy(0, far).start()
        double_copy(1, far).start()
        for way in range(2):
            plane_copy(way, far, near).start()

    def relation_known(row):
        for way in range(2):
            plane_copy(way, row, near).start()

    def relation_relay(row):
        plane_copy(0, row, near_x).wait_recv()
        relay_copy(0, row, near_x).start()
        plane_copy(1, row, near_y).wait_recv()
        relay_copy(1, row, near_y).start()

    def relation_end():
        for row in known_rows:
            for way in range(2):
                relay_copy(way, row, near_xy).wait_recv()

    span = 256 if rows_here % 256 == 0 else rows_here

    def start_totals(index):
        first = pl.multiple_of(index * span, span)
        rows_of = first + lax.broadcasted_iota(jnp.int32, (span, slots), 0)
        count = jnp.zeros((span, slots), jnp.float32)
        for beside in range(near_size):
            for there in range(far_size):
                for group in range(groups):
                    targets = own_ids[beside, there][group : group + 1, :slots]
                    count += (rows_of == targets).astype(jnp.float32)
        count = jnp.sum(count, axis=1, keepdims=True)
        weight = jnp.transpose(weights[:, pl.ds(first, span)])[:, :1] * count
        own = entities[pl.ds(first, span)]
        totals[pl.ds(first, span)] = weight * own * jnp.abs(own)

    def norm_copy(which, step):
        peer = lax.rem(part_here + step, parts)
        held = s["rel_all" if which else "ent_all"].at[part_here]
        return send(held, held, s["norm_ss"].at[which, step], s["norm_rs"].at[which, step], peer, axis="dim")

    def norm_start(which):
        values = rel_out if which else totals
        held = s["rel_all" if which else "ent_all"]

        @pl.loop(0, values.shape[0] // span)
        def _(index):
            first = pl.multiple_of(index * span, span)
            block = values[pl.ds(first, span)].astype(jnp.float32)
            square = jnp.sum(block * block, axis=1, keepdims=True)
            held[part_here, :, pl.ds(first, span)] = jnp.transpose(jnp.broadcast_to(square, (span, 8)))

        for step in range(1, parts):
            norm_copy(which, step).start()

    def norm_end(which):
        held = s["rel_all" if which else "ent_all"]
        for step in range(1, parts):
            norm_copy(which, step).wait()
        total = held[0]
        for other in range(1, parts):
            total += held[other]
        (rel_squares if which else ent_squares)[...] = total

    @pl.loop(0, far_size * near_size)
    def _(index):
        look_up(0, index)

    for group in range(1, groups):

        @pl.loop(0, far_size)
        def _(index):
            @pl.loop(0, near_size)
            def _(part):
                look_up(group, index * near_size + part)

            merge(group - 1, index)

    @pl.loop(0, rows_here // span)
    def _(index):
        start_totals(index)

    last = groups - 1
    early = far_size // 2 if groups > 1 else far_size

    @pl.loop(0, early)
    def _(index):
        merge(last, index)

    for group in range(last):
        compute(group)
        if group == 0:

            @pl.loop(early, far_size)
            def _(index):
                merge(last, index)

        give_blocks(group)
        for index in range(far_size - 1):
            give_start(group, index)
        if in_kernel_sum:
            relation_parts(group)

    if last > 0:
        spread(0, 0)
    compute(last)
    if in_kernel_sum:
        if last > 0:
            spread(0, 1)
        give_blocks(last)
        relation_parts(last)
        relation_halve()
        give_start(last, 0)
        if last > 0:
            span_of(spread, 0, 2, 4)
        relation_across()
        span_of(spread, last, 0, 2)
        relation_share()
        give_start(last, 1)
        give_start(last, 2)
        double_copy(1, beside_far).wait_recv()
        relation_known(beside_far)
        double_copy(0, across_far).wait_recv()
        pass_copy(across_far).start()
        relation_known(across_far)
        relation_relay(far)
        pass_copy(diagonal_far).wait_recv()
        relation_known(diagonal_far)
        relation_relay(beside_far)
        spread(last, 2)
        relation_relay(across_far)
        if last > 0:
            span_of(add_up, 0, 0, 2)
        spread(last, 3)
        relation_relay(diagonal_far)
        if last > 0:
            span_of(add_up, 0, 2, 4)
        span_of(add_up, last, 0, 2)
        relation_end()
        norm_start(1)
        span_of(add_up, last, 2, 4)
        norm_start(0)
        norm_end(1)
    else:
        give_blocks(last)
        for index in range(far_size - 1):
            give_start(last, index)
        for group in range(groups):

            @pl.loop(1 if group == 0 and last > 0 else 0, far_size)
            def _(index):
                spread(group, index)

        for group in range(groups):
            add_up_all(group)
        norm_start(0)
        rel_squares[...] = jnp.zeros_like(rel_squares)
    norm_end(0)

    for group in range(groups):
        for step in range(1, far_size):
            there = lax.rem(far + step, far_size)
            far_copy(group, there, 0).wait_send()
            give_copy(group, there, 0).wait_send()
        for step in range(1, parts):
            part_copy(group, step).wait_send()
        for step in range(1, near_size):

            @pl.loop(0, far_size)
            def _(there):
                near_copy(group, step, there).wait_send()
                hand_copy(group, step, there).wait_send()

    if in_kernel_sum:
        for step in range(1, near_size):
            for group in range(groups):
                tiles_copy(group, step).wait_send()
        for index in range(2):
            halve_copy(index).wait_send()
            double_copy(index, far).wait_send()
        across_copy().wait_send()
        pass_copy(across_far).wait_send()
        for row in known_rows:
            for way in range(2):
                plane_copy(way, row, near).wait_send()
                relay_copy(way, row, near).wait_send()


def sums_in_kernel(columns, near_size, far_size):
    return near_size == 4 and far_size == 4 and columns % (2 * BLK * near_size) == 0


def exchange_step(inputs, sizes, collective_id):
    near_size, far_size, groups, slots, merged, group_len, width_neg, rel_count = sizes
    rows_here, columns = inputs[0].shape
    parts = lax.axis_size("dim")
    dma = pltpu.SemaphoreType.DMA
    low = jnp.bfloat16
    vmem = pl.BlockSpec(memory_space=pltpu.VMEM)
    request_count = 2 * group_len + width_neg
    in_kernel_sum = sums_in_kernel(columns, near_size, far_size)
    scratch = {
        "table": pltpu.VMEM((rows_here, columns), low),
        "ent_all": pltpu.VMEM((parts, 8, rows_here), jnp.float32),
        "near_out": pltpu.VMEM((groups, near_size, far_size, slots, columns), low),
        "near_in": pltpu.VMEM((groups, far_size, near_size, slots, columns), low),
        "far_out": pltpu.VMEM((groups, far_size, merged, columns), low),
        "arrived": pltpu.VMEM((groups, far_size, merged, columns), low),
        "rows": pltpu.VMEM((request_count, columns), low),
        "grads": pltpu.VMEM((request_count, columns), low),
        "query": pltpu.VMEM((group_len, columns), low),
        "probe": pltpu.VMEM((group_len, columns), low),
        "part_all": pltpu.VMEM((groups, parts, group_len, 2 * width_neg + 128), low),
        "give_out": pltpu.VMEM((groups, far_size, merged, columns), low),
        "give_in": pltpu.VMEM((groups, far_size, merged, columns), low),
        "hand_out": pltpu.VMEM((groups, far_size, near_size, slots, columns), low),
        "hand_in": pltpu.VMEM((groups, far_size, near_size, slots, columns), low),
    }
    for name, shape in (
        ("near", (groups, near_size, far_size)), ("far", (groups, far_size)),
        ("part", (groups, parts)), ("give", (groups, far_size)), ("norm", (2, parts)),
        ("hand", (groups, near_size, far_size)),
    ):
        scratch[name + "_ss"] = dma(shape)
        scratch[name + "_rs"] = dma(shape)
    if in_kernel_sum:
        width = columns // near_size
        scratch["rel_all"] = pltpu.VMEM((parts, 8, rel_count), jnp.float32)
        scratch["tiles_out"] = pltpu.VMEM((near_size, groups * group_len, width), low)
        scratch["tiles_in"] = pltpu.VMEM((near_size, groups * group_len, width), low)
        scratch["rel_part"] = pltpu.VMEM((rel_count, width), low)
        scratch["share_in"] = pltpu.VMEM((3, rel_count // far_size, width), low)
        scratch["share_out"] = pltpu.VMEM((rel_count // far_size, width), low)
        for name, shape in (
            ("tiles", (groups, near_size)), ("halve", (2,)), ("double", (3,)), ("pass", (1,)),
            ("pg", (2, far_size)), ("relay", (2, far_size)),
        ):
            scratch[name + "_ss"] = dma(shape)
            scratch[name + "_rs"] = dma(shape)
    names = tuple(scratch)
    rel_rows_out = rel_count if in_kernel_sum else groups * group_len

    def kernel(*refs):
        step_kernel(sizes, refs[:7], refs[7:11], dict(zip(names, refs[11:])))

    return pl.pallas_call(
        kernel,
        name="exchange_step",
        out_shape=(
            jax.ShapeDtypeStruct((rows_here, columns), jnp.float32),
            jax.ShapeDtypeStruct((8, rows_here), jnp.float32),
            jax.ShapeDtypeStruct((rel_rows_out, columns), low),
            jax.ShapeDtypeStruct((8, rel_count), jnp.float32),
        ),
        in_specs=[vmem] * 7,
        out_specs=(vmem,) * 4,
        scratch_shapes=list(scratch.values()),
        compiler_params=pltpu.CompilerParams(
            collective_id=collective_id, has_side_effects=True, vmem_limit_bytes=VMEM_LIMIT
        ),
    )(*inputs)


def placement_of(wanted_row, rows_here, sizes):
    near_size, far_size, slots = sizes
    owners = near_size * far_size
    request_count = wanted_row.shape[0]
    owner_of = wanted_row // rows_here
    owner_hits = (owner_of[:, None] == jnp.arange(owners, dtype=jnp.int32)[None, :]).astype(
        jnp.bfloat16
    )
    order = jnp.arange(request_count, dtype=jnp.int32)
    earlier = (order[:, None] > order[None, :]).astype(jnp.bfloat16)
    before = jnp.dot(earlier, owner_hits, preferred_element_type=jnp.float32)
    slot_rank = jnp.sum(before * owner_hits.astype(jnp.float32), axis=-1).astype(jnp.int32)
    plane_of = owner_of // near_size
    same_plane = (
        plane_of[:, None] == (jnp.arange(owners, dtype=jnp.int32) // near_size)[None, :]
    ).astype(jnp.float32)
    plane_rank = jnp.sum(before * same_plane, axis=-1).astype(jnp.int32)
    slot_flat = owner_of * slots + slot_rank
    at_slot = slot_flat[:, None] == jnp.arange(owners * slots, dtype=jnp.int32)[None, :]
    local_row = wanted_row - owner_of * rows_here
    slot_ids = jnp.sum(jnp.where(at_slot, local_row[:, None] + 1, 0), axis=0) - 1
    slot_map = jnp.sum(jnp.where(at_slot, plane_rank[:, None] + 1, 0), axis=0) - 1
    return (plane_of, plane_rank, slot_ids, slot_map)


def teams(near_size, far_size):
    near = [[row * near_size + place for place in range(near_size)] for row in range(far_size)]
    far = [[row * near_size + place for row in range(far_size)] for place in range(near_size)]
    return (near, far)


def sum_relations(rel_rows, near_ids, rel_count, near, far):
    near_size, far_size = len(far), len(near)
    row_count, columns = rel_rows.shape
    tiles = rel_rows.reshape(row_count, near_size, columns // near_size).transpose(1, 0, 2)
    tiles = lax.all_to_all(
        tiles, "ent", split_axis=0, concat_axis=0, axis_index_groups=near, tiled=True
    )
    hits = (near_ids[:, None] == jnp.arange(rel_count, dtype=jnp.int32)[None, :]).astype(
        jnp.bfloat16
    )
    part = contract_first(hits, tiles.reshape(near_size * row_count, columns // near_size)).astype(
        jnp.bfloat16
    )
    share = lax.psum_scatter(
        part, "ent", scatter_dimension=0, axis_index_groups=far, tiled=True
    )
    whole = lax.all_gather(share, "ent", axis=0)
    whole = whole.reshape(far_size, near_size, rel_count // far_size, columns // near_size)
    return whole.transpose(0, 2, 1, 3).reshape(rel_count, columns)


def adagrad(table, state, grad, squares):
    new_state = state + squares / (2 * RANK)
    scale = LEARN_RATE / jnp.sqrt(new_state)
    return table - grad * scale[:, None]


def per_device(entities, ent_state, buckets, relations, rel_state, triples, negatives):
    owners = lax.axis_size("ent")
    rows_here, columns_here = entities.shape
    rel_count = relations.shape[0]
    groups_here, width_neg = negatives.shape
    group_len = triples.shape[1] // groups_here
    request_count = 2 * group_len + width_neg
    slots = 8 * ((request_count + 3 * owners - 1) // (3 * owners))
    near_size = 4 if owners % 4 == 0 else 1
    far_size = owners // near_size
    most = min(near_size * slots, request_count)
    few = min(most, 16 * ((19 * slots + 127) // 128))
    head_ids = triples[0].reshape(groups_here, group_len)
    tail_ids = triples[2].reshape(groups_here, group_len)
    wanted = jnp.concatenate([head_ids, tail_ids, negatives], axis=1)
    placed = [
        placement_of(wanted[index], rows_here, (near_size, far_size, slots))
        for index in range(groups_here)
    ]
    plane_of = jnp.stack([each[0] for each in placed])
    plane_rank = jnp.stack([each[1] for each in placed])
    slot_ids = jnp.stack([each[2] for each in placed])
    slot_ids = slot_ids.reshape(groups_here, far_size, near_size, slots).transpose(1, 2, 0, 3)
    slot_ids = jnp.pad(
        slot_ids, ((0, 0), (0, 0), (0, 8 - groups_here), (0, 128 - slots)), constant_values=-1
    )
    slot_maps = jnp.stack([each[3] for each in placed])
    slot_maps = slot_maps.reshape(groups_here, far_size, near_size * slots).transpose(1, 0, 2)
    slot_maps = jnp.pad(slot_maps, ((0, 0), (0, 8 - groups_here), (0, 0)), constant_values=-1)
    rel_rows = jnp.take(relations, triples[1], axis=0, mode="clip").astype(jnp.bfloat16)
    rel_ids = jnp.broadcast_to(triples[1][None, :], (8, triples.shape[1]))

    own_ids, line_maps, plane_rel = share_ids(slot_ids, slot_maps, rel_ids, (near_size, far_size))
    longest = jnp.max(own_ids[:, 0, 7])
    place = jnp.pad(
        jnp.concatenate([plane_of, plane_rank]), ((0, 8 - 2 * groups_here), (0, 0)), constant_values=-1
    )

    def run(merged, collective_id):
        sizes = (near_size, far_size, groups_here, slots, merged, group_len, width_neg, rel_count)
        return lambda *inputs: exchange_step(inputs, sizes, collective_id)

    weights = 3.0 * REG_WEIGHT * (buckets.astype(jnp.float32) + 1.0)
    weights = jnp.broadcast_to(weights[None, :], (8, rows_here))
    operands = (entities, own_ids, line_maps, place, rel_rows, plane_rel, weights)
    totals, ent_all, rel_grad, rel_all = lax.cond(
        longest <= few, run(few, 0), run(most, 1), *operands
    )
    if rel_grad.shape[0] != rel_count:
        near, far = teams(near_size, far_size)
        near_ids = lax.all_gather(triples[1], "ent", axis_index_groups=near, tiled=True)
        rel_grad = sum_relations(rel_grad, near_ids, rel_count, near, far)
        rel_all = lax.psum(jnp.sum(rel_grad.astype(jnp.float32) ** 2, axis=-1), "dim")[None]
    rel_grad = rel_grad.astype(jnp.float32)
    new_relations = adagrad(relations, rel_state, rel_grad, rel_all[0])
    new_entities = adagrad(entities, ent_state, totals, ent_all[0])
    return (new_entities, new_relations)


def solution(mesh):
    placed = (
        P("ent", "dim"),
        P("ent"),
        P("ent"),
        P(None, "dim"),
        P(),
        P(None, "ent"),
        P("ent", None),
    )
    return jax.shard_map(
        per_device,
        mesh=mesh,
        in_specs=placed,
        out_specs=(P("ent", "dim"), P(None, "dim")),
        check_vma=False,
    )
```
